32 devices in a mesh: groups: 1, ctx: 32 (over z, y, x, core).
Axes of the slice: x: 2, y: 2, z: 4, core: 2. Of those that a mesh axis runs over, the one named last changes fastest.
Arguments:
- prefill_query: bfloat16 [1024, 32, 576], P('groups', 'ctx'), may hold values from -1000 to 1000
- prefill_latent: bfloat16 [1024, 576], P(('groups', 'ctx')), may hold values from -6 to 6
- decode_query: bfloat16 [2, 32, 576], P('groups'), may hold values from -1000 to 1000
- cache: bfloat16 [2, 16384, 576], P('groups', 'ctx'), may hold values from -6 to 6
- lengths: int32 [2], P('groups'), may hold values from 2049 to 16384
- page_table: int32 [64, 2], P('groups'), may hold values from 0 to 31, as said below
Outputs:
- prefill_out: bfloat16 [1024, 32, 512], P('groups', 'ctx')
- decode_out: bfloat16 [2, 32, 512], P('groups', 'ctx')
The draws below stay inside these ranges and needn't reach their ends.
Inputs may be any that keep to these rules, and one draw needn't show every extreme that they name: `page_table`: row p names the device (column 0, below 32) and the pool slot (column 1, below 16) that take latent page p; no two rows name the same pair.
All inputs are finite; a program needn't handle non-finite values.
Results may differ from the reference program's by a relative error of at most 0.0049.
Values may be sent and summed in bfloat16 or wider, within the bound.
A program may use at most 64 MiB of HBM per device.

```python
import jax
import jax.numpy as jnp
from jax import lax

D_LAT = 512
D_ROPE = 64
PAGE = 16
POOL = 16
SPAN = 1024
REQ = 2
HEADS = 32
CTXLEN = 16384
NPAGES = 64
N_CTX = 32


SCALE = 192.0 ** (-0.5)


def cache_block(key, request, block):
    sub_key = jax.random.fold_in(jax.random.fold_in(jax.random.fold_in(key, 501), request), block)
    raw = jax.random.normal(sub_key, (64, D_LAT + D_ROPE), jnp.float32)
    return jnp.clip(raw, -6.0, 6.0).astype(jnp.bfloat16).astype(jnp.float32)


def cache_row(key, request, position):
    return cache_block(key, request, position // 64)[position % 64]


def latent_matrix(key):
    raw = jax.random.normal(jax.random.fold_in(key, 502), (SPAN, D_LAT + D_ROPE), jnp.float32)
    return jnp.clip(raw, -6.0, 6.0).astype(jnp.bfloat16).astype(jnp.float32)


def aligned(first, second, strength):
    self_first = jnp.sum(first * first, axis=-1)
    self_second = jnp.sum(second * second, axis=-1)
    cross = jnp.sum(first * second, axis=-1)
    coefficient = (strength * (self_first - cross) - 2.0 / SCALE) / (self_second - cross)
    return strength[..., None] * first + coefficient[..., None] * second


def strength_table():
    return jnp.array([3.0, 5.0, 8.0], jnp.float32) * (576.0 / (D_LAT + D_ROPE))


def prefill_built(key):
    latent = latent_matrix(key)
    picked = HEADS // 16
    row_index = jnp.arange(SPAN)[:, None]
    head_index = jnp.arange(picked)[None, :]
    other = jax.random.randint(jax.random.fold_in(key, 512), (SPAN, picked), 0, SPAN) % jnp.maximum(row_index, 1)
    strength = strength_table()[(head_index + row_index) % 3]
    first = latent[jnp.broadcast_to(row_index, (SPAN, picked))]
    second = latent[other]
    built = aligned(first, second, strength)
    chosen = jnp.broadcast_to(row_index % 64 == 63, (SPAN, picked))
    return (built, chosen)


def decode_built(key):
    picked = HEADS // 16
    reach = CTXLEN // 8
    first_pos = jax.random.randint(jax.random.fold_in(key, 522), (REQ, picked), 0, reach)
    step_pos = jax.random.randint(jax.random.fold_in(key, 523), (REQ, picked), 1, reach)
    second_pos = (first_pos + step_pos) % reach
    request_index = jnp.broadcast_to(jnp.arange(REQ)[:, None], (REQ, picked))
    head_index = jnp.arange(picked)[None, :]
    row_fetch = jax.vmap(jax.vmap(lambda request, position: cache_row(key, request, position)))
    first = row_fetch(request_index, first_pos)
    second = row_fetch(request_index, second_pos)
    strength = strength_table()[(head_index + request_index) % 3]
    return aligned(first, second, strength)


def draw_cache(key, part):
    blocks = CTXLEN // 64
    full = jax.vmap(lambda request: jax.vmap(lambda block: cache_block(key, request, block))(jnp.arange(blocks)))(jnp.arange(REQ))
    return full.reshape(REQ, CTXLEN, D_LAT + D_ROPE).astype(jnp.bfloat16)


def draw_prefill_latent(key, part):
    return latent_matrix(key).astype(jnp.bfloat16)


def draw_prefill_query(key, part):
    width = D_LAT + D_ROPE
    plain = 2.0 * jnp.clip(jax.random.normal(jax.random.fold_in(key, 513), (SPAN, HEADS, width), jnp.float32), -6.0, 6.0)
    built, chosen = prefill_built(key)
    query = plain.at[:, ::16, :].set(jnp.where(chosen[..., None], built, plain[:, ::16, :]))
    return jnp.clip(query, -1000.0, 1000.0).astype(jnp.bfloat16)


def draw_decode_query(key, part):
    width = D_LAT + D_ROPE
    plain = 2.0 * jnp.clip(jax.random.normal(jax.random.fold_in(key, 524), (REQ, HEADS, width), jnp.float32), -6.0, 6.0)
    query = plain.at[:, ::16, :].set(decode_built(key))
    return jnp.clip(query, -1000.0, 1000.0).astype(jnp.bfloat16)


def draw_page_table(key, part):
    order = jax.random.permutation(jax.random.fold_in(key, 531), N_CTX * POOL)[:NPAGES]
    return jnp.stack([order // POOL, order % POOL], axis=1).astype(jnp.int32)


def setup_inputs(seed: int = 0, part: int = 0) -> dict:
    keys = jax.random.split(jax.random.key(seed), 7)
    own_keys = jax.random.split(jax.random.fold_in(keys[6], part), 7)
    prefill_query = draw_prefill_query(jax.random.fold_in(jax.random.fold_in(keys[6], part), 71), part)
    prefill_latent = draw_prefill_latent(jax.random.fold_in(jax.random.fold_in(keys[6], part), 71), part)
    decode_query = draw_decode_query(jax.random.fold_in(jax.random.fold_in(keys[6], part), 71), part)
    cache = draw_cache(jax.random.fold_in(jax.random.fold_in(keys[6], part), 71), part)
    lengths = jax.random.randint(own_keys[4], (REQ,), CTXLEN // 8 + 1, CTXLEN + 1).astype(jnp.int32)
    page_table = draw_page_table(jax.random.fold_in(jax.random.fold_in(keys[6], part), 71), part)
    return dict(prefill_query=prefill_query, prefill_latent=prefill_latent, decode_query=decode_query, cache=cache, lengths=lengths, page_table=page_table)


SCALE = 192.0 ** -0.5
NEG = -1.0e30


def softmax_values(scores, allowed, values):
    masked = jnp.where(allowed, scores, NEG)
    top_score = jnp.max(masked, axis=-1, keepdims=True)
    weights = jnp.where(allowed, jnp.exp(scores - top_score), 0.0)
    weight_sum = jnp.sum(weights, axis=-1, keepdims=True)
    mixed = jnp.dot(weights.astype(jnp.bfloat16), values, preferred_element_type=jnp.float32)
    return mixed / weight_sum


def reference(prefill_query, prefill_latent, decode_query, cache, lengths, page_table):
    latent_values = prefill_latent[:, :D_LAT]
    causal = jnp.arange(SPAN, dtype=jnp.int32)[:, None] >= jnp.arange(SPAN, dtype=jnp.int32)[None, :]

    def one_head(queries):
        scores = jnp.dot(queries, prefill_latent.T, preferred_element_type=jnp.float32) * SCALE
        return softmax_values(scores, causal, latent_values).astype(jnp.bfloat16)

    per_head = lax.map(one_head, jnp.swapaxes(prefill_query, 0, 1))
    prefill_out = jnp.swapaxes(per_head, 0, 1)

    page_request = (page_table[:, 0] * POOL + page_table[:, 1]) % REQ
    token_request = jnp.repeat(page_request, PAGE)
    positions = jnp.arange(CTXLEN, dtype=jnp.int32)

    def one_request(request):
        queries = decode_query[request]
        rows_cache = cache[request]
        cache_scores = jnp.dot(queries, rows_cache.T, preferred_element_type=jnp.float32) * SCALE
        page_scores = jnp.dot(queries, prefill_latent.T, preferred_element_type=jnp.float32) * SCALE
        scores = jnp.concatenate([cache_scores, page_scores], axis=1)
        allowed = jnp.concatenate([positions < lengths[request], token_request == request])[None, :]
        values = jnp.concatenate([rows_cache[:, :D_LAT], latent_values], axis=0)
        return softmax_values(scores, allowed, values).astype(jnp.bfloat16)

    decode_out = lax.map(one_request, jnp.arange(REQ, dtype=jnp.int32))
    return prefill_out, decode_out
```

```python
import functools

import jax
import jax.numpy as jnp
from jax import lax
from jax.experimental import pallas as pl
from jax.experimental.pallas import tpu as pltpu
from jax.sharding import PartitionSpec as P

D_LAT = 512
PAGE = 16
POOL = 16
REQ = 2

SCALE = 192.0 ** (-0.5)
NEG = -1e30
MSG = D_LAT + 128
NT = (((1,), (1,)), ((), ()))


def kernel(
    n,
    qt_hbm,
    lat_hbm,
    dq_hbm,
    ct_hbm,
    len_hbm,
    pt_hbm,
    pout_ref,
    dout_ref,
    held,
    dq_ref,
    qt,
    q,
    ct,
    len_ref,
    pt_ref,
    parts,
    mate,
    joined,
    moved,
    local_sem,
    send_sem,
    column_sem,
    plane_sem,
    diag_sem,
    pair_sem,
    part_sem,
    mate_sem,
    ready_sem,
    near_sem,
    reach_sem,
):
    me = lax.axis_index("ctx")
    line = n // 8
    core = me % 2
    x = (me // 2) % 2
    y = (me // 4) % 2
    z = me // 8
    far_x, far_y = 1 - x, 1 - y
    rows = lat_hbm.shape[0]
    heads = dq_ref.shape[1]
    chips = n // 2
    chip = me // 2
    span = qt.shape[1]
    cache_dev = ct.shape[2]
    split = rows // 2 if rows % 32 == 0 else rows

    def block(bz, by, bx, bc):
        return ((bz * 2 + by) * 2 + bx) * 2 + bc

    x_peer = block(z, y, far_x, core)
    y_peer = block(z, far_y, x, core)
    pair = block(z, y, x, 1 - core)

    def local(index, source, target):
        copy = pltpu.make_async_copy(source, target, local_sem.at[index])
        copy.start()
        return copy

    own_copy = local(0, lat_hbm, held.at[me])
    c_copy = local(1, ct_hbm, ct)
    d_copy = local(2, dq_hbm, dq_ref)
    len_copy = local(3, len_hbm, len_ref)
    pt_copy = local(4, pt_hbm, pt_ref)
    q_copy = local(5, qt_hbm, qt)

    barrier = pltpu.get_barrier_semaphore()
    peers = ((x, x_peer), (y, y_peer), (core, pair))
    for side, target in peers:

        @pl.when(side == 0)
        def _(target=target):
            pl.semaphore_signal(barrier, inc=1, device_id={"ctx": target})

    def greet(bz, carry):
        pl.semaphore_signal(barrier, inc=1, device_id={"ctx": block(bz, y, x, core)})
        return carry

    lax.fori_loop(z + 1, line, greet, 0)

    @pl.when((z == 0) & (y == 0))
    def _():
        pl.semaphore_signal(barrier, inc=1, device_id={"ctx": block(line - 1, far_y, far_x, core)})

    def both(distance, act):
        if distance == 0:
            act(z)
            return
        pl.when(z + distance < line)(lambda: act(z + distance))
        pl.when(z >= distance)(lambda: act(z - distance))

    def move(index, recv, target, part=None):
        ref = held.at[index]
        if part == 0:
            ref = held.at[index, pl.ds(0, split)]
        if part == 1:
            ref = held.at[index, pl.ds(split, rows - split)]
        pltpu.make_async_remote_copy(
            src_ref=ref, dst_ref=ref, send_sem=send_sem, recv_sem=recv, device_id={"ctx": target}
        ).start()

    def blocks_wait(sem, count):
        ref = held.at[pl.ds(0, count)]
        pltpu.make_async_copy(ref, ref, sem).wait()

    def to_pair(bz, by, bx):
        index = block(bz, by, bx, core)
        move(index, pair_sem.at[bz], pair)

    def spread(bz):
        index = block(bz, y, x, core)
        move(index, plane_sem.at[bz], x_peer)
        move(index, plane_sem.at[bz], y_peer)
        to_pair(bz, y, x)

    def column_step(bz):
        blocks_wait(column_sem.at[bz], 1)
        spread(bz)

    def relay_y(bz):
        if split < rows:
            move(block(bz, y, far_x, core), diag_sem.at[bz], y_peer, 1)

    def relay_x(bz):
        move(block(bz, far_y, x, core), diag_sem.at[bz], x_peer, 0)

    def plane_step(bz, first=False):
        blocks_wait(plane_sem.at[bz], 2)
        if first:
            pl.when(y == 0)(lambda: move(block(bz, y, far_x, core), diag_sem.at[bz], y_peer))
        else:
            relay_y(bz)
            relay_x(bz)
        to_pair(bz, y, far_x)
        to_pair(bz, far_y, x)

    def diag_step(bz):
        blocks_wait(diag_sem.at[bz], 1)
        to_pair(bz, far_y, far_x)

    def up_step(distance):
        @pl.when(z + distance < line)
        def _():
            pl.semaphore_wait(ready_sem.at[z + distance], 1)
            own(column_sem.at[z], block(z + distance, y, x, core))

    def own(recv, target):
        pltpu.make_async_remote_copy(
            src_ref=lat_hbm,
            dst_ref=held.at[me],
            send_sem=send_sem,
            recv_sem=recv,
            device_id={"ctx": target},
        ).start()

    def down(bz, carry):
        own(column_sem.at[z], block(bz, y, x, core))
        return carry

    def ready(bz, carry):
        pl.semaphore_signal(ready_sem.at[z], inc=1, device_id={"ctx": block(bz, y, x, core)})
        return carry

    def reach(target, carry):
        pl.semaphore_signal(reach_sem, inc=1, device_id={"ctx": target * 2 + core})
        return carry

    direct = jnp.where(z == line - 1, y, 0)
    entered = z + direct + x + y + core
    pl.when(entered > 0)(lambda: pl.semaphore_wait(barrier, entered))
    lax.fori_loop(0, z, down, 0)

    @pl.when((z == line - 1) & (y == 1))
    def _():
        own(diag_sem.at[z], block(0, far_y, far_x, core))

    plane_sems = (plane_sem, plane_sem, pair_sem)
    for step, (side, target) in enumerate(peers):

        @pl.when(side == 1)
        def _(target=target, step=step):
            pl.semaphore_signal(near_sem.at[step], inc=1, device_id={"ctx": target})
            own(plane_sems[step].at[z], target)

    lax.fori_loop(0, z, ready, 0)
    for step, (side, target) in enumerate(peers):

        @pl.when(side == 0)
        def _(target=target, step=step):
            pl.semaphore_wait(near_sem.at[step], 1)
            own(plane_sems[step].at[z], target)
            if step == 0:
                pl.semaphore_signal(near_sem.at[0], inc=1, device_id={"ctx": target})

    own_copy.wait()
    c_copy.wait()
    d_copy.wait()
    len_copy.wait()
    pt_copy.wait()
    latent = held[me]
    row_page = (me * rows + lax.broadcasted_iota(jnp.int32, (1, rows), 1)) // PAGE
    first_page = me * rows // PAGE
    request_of = jnp.zeros((1, rows), jnp.int32)
    for p in range(max(1, rows // PAGE)):
        page = first_page + p
        request = (pt_ref[0, page] * POOL + pt_ref[1, page]) % REQ
        request_of = jnp.where(row_page == page, request, request_of)
    positions = me * cache_dev + lax.broadcasted_iota(jnp.int32, (1, cache_dev), 1)
    for r in range(REQ):
        queries = dq_ref[r]
        keys = ct[r]
        scores = jnp.dot(queries, keys, preferred_element_type=jnp.float32) * SCALE
        page_scores = (
            lax.dot_general(queries, latent, NT, preferred_element_type=jnp.float32) * SCALE
        )
        ok = positions < len_ref[r]
        page_ok = request_of == r
        scores = jnp.where(ok, scores, NEG)
        page_scores = jnp.where(page_ok, page_scores, NEG)
        top = jnp.maximum(
            jnp.max(scores, axis=1, keepdims=True), jnp.max(page_scores, axis=1, keepdims=True)
        )
        weights = jnp.where(ok, jnp.exp(scores - top), 0.0)
        page_weights = jnp.where(page_ok, jnp.exp(page_scores - top), 0.0)
        total = jnp.sum(weights, axis=1, keepdims=True) + jnp.sum(
            page_weights, axis=1, keepdims=True
        )
        mixed = lax.dot_general(
            weights.astype(jnp.bfloat16), keys[:D_LAT], NT, preferred_element_type=jnp.float32
        ) + jnp.dot(
            page_weights.astype(jnp.bfloat16),
            latent[:, :D_LAT],
            preferred_element_type=jnp.float32,
        )
        lane = lax.broadcasted_iota(jnp.int32, (heads, 128), 1)
        tail = jnp.where(lane < 64, top, total)
        parts[:, :, :, r * MSG : r * MSG + D_LAT] = mixed.reshape(chips, 2, 1, D_LAT)
        parts[:, :, :, r * MSG + D_LAT : (r + 1) * MSG] = tail.reshape(chips, 2, 1, 128)

    mate_copy = pltpu.make_async_remote_copy(
        src_ref=parts.at[:, 1 - core],
        dst_ref=mate,
        send_sem=mate_sem.at[0],
        recv_sem=mate_sem.at[1],
        device_id={"ctx": pair},
    )
    mate_copy.start()

    @pl.when(x == 1)
    def _():
        pl.semaphore_wait(near_sem.at[0], 1)

    pl.semaphore_signal(near_sem.at[3], inc=1, device_id={"ctx": y_peer})

    def part_copy(target):
        return pltpu.make_async_remote_copy(
            src_ref=joined.at[target],
            dst_ref=moved.at[chip],
            send_sem=part_sem.at[0],
            recv_sem=part_sem.at[1],
            device_id={"ctx": target * 2 + core},
        )

    def send_part(target, carry):
        part_copy(target).start()
        return carry

    def join():
        mate_copy.wait_recv()
        for r in range(REQ):
            mine = parts[:, core, :, r * MSG : (r + 1) * MSG].reshape(chips, MSG)
            other = mate[:, :, r * MSG : (r + 1) * MSG].reshape(chips, MSG)
            top_mine = mine[:, D_LAT : D_LAT + 1]
            top_other = other[:, D_LAT : D_LAT + 1]
            top = jnp.maximum(top_mine, top_other)
            sum_both = mine * jnp.exp(top_mine - top) + other * jnp.exp(top_other - top)
            lane = lax.broadcasted_iota(jnp.int32, (chips, 128), 1)
            tail = jnp.where(lane < 64, top, sum_both[:, D_LAT:])
            joined[:, :, r * MSG : r * MSG + D_LAT] = sum_both[:, :D_LAT].reshape(chips, 1, D_LAT)
            joined[:, :, r * MSG + D_LAT : (r + 1) * MSG] = tail.reshape(chips, 1, 128)
        moved[chip] = joined[chip]

    quarter = span // 4
    group = n // 4

    def attend(i, first, last):
        start, count = i * quarter, (last - first) * quarter
        keys = held[first * group : last * group].reshape(count, held.shape[2])
        scores = lax.dot_general(
            q[start : start + quarter], keys, NT, preferred_element_type=jnp.float32
        )
        if last == i + 1:
            row = start + lax.broadcasted_iota(jnp.int32, (quarter, count), 0)
            col = first * quarter + lax.broadcasted_iota(jnp.int32, (quarter, count), 1)
            scores = jnp.where(col <= row, scores, NEG)
        top = jnp.max(scores, axis=1, keepdims=True)
        weights = jnp.exp((scores - top) * SCALE)
        total = jnp.sum(weights, axis=1, keepdims=True)
        mixed = jnp.dot(
            weights.astype(jnp.bfloat16), keys[:, :D_LAT], preferred_element_type=jnp.float32
        )
        return top, total, mixed

    def finish(i, total, mixed):
        pout_ref[i * quarter : (i + 1) * quarter, :] = (mixed / total).astype(jnp.bfloat16)

    def await_group(p):
        for bz in range(p * (line // 4), (p + 1) * (line // 4)):
            blocks_wait(pair_sem.at[bz], 4)

    def transpose_queries():
        q_copy.wait()
        for start in range(0, span, 128):
            q[start : start + 128, :] = qt[:, start : start + 128].T

    transpose_queries()
    join()
    pl.semaphore_wait(near_sem.at[3], 1)
    lax.fori_loop(0, 4 * z, send_part, 0)
    lax.fori_loop(0, 4 * z, reach, 0)
    for step in range(1, line):
        up_step(step)
    for step in range(1, line):
        both(step, column_step)
        if step == 1:
            plane_step(z)
    both(1, plane_step)
    diag_step(z)
    pl.when(z < line - 1)(lambda: pl.semaphore_wait(reach_sem, 4 * (line - 1 - z)))
    lax.fori_loop(4 * z, chip, send_part, 0)
    lax.fori_loop(chip + 1, chips, send_part, 0)
    for step in range(2, line - 1):
        both(step, plane_step)
    pl.when(z == 0)(lambda: plane_step(line - 1, True))
    pl.when(z == line - 1)(lambda: plane_step(0))
    for step in range(1, line):
        both(step, diag_step)

    for p in range(4):
        await_group(p)
    parts_all = moved.at[pl.ds(0, chips - 1)]
    pltpu.make_async_copy(parts_all, parts_all, part_sem.at[1]).wait()
    for r in range(REQ):
        piece = moved[:, :, r * MSG : (r + 1) * MSG].reshape(chips, MSG)
        best = piece[:, D_LAT : D_LAT + 1]
        mass = piece[:, D_LAT + 64 : D_LAT + 65]
        factor = jnp.exp(best - jnp.max(best, axis=0, keepdims=True))
        own_sum = jnp.sum(mass * factor, axis=0, keepdims=True)
        own_out = jnp.sum(piece[:, :D_LAT] * factor, axis=0, keepdims=True)
        dout_ref[r : r + 1, :] = (own_out / own_sum).astype(jnp.bfloat16)

    for i in range(4):
        _, total, mixed = attend(i, 0, i + 1)
        finish(i, total, mixed)

    blocks_wait(send_sem, n - 2)
    pl.when((z > 0) | (y == 0))(lambda: blocks_wait(send_sem, 1))
    pl.when((z == line - 1) & (y == 1))(lambda: blocks_wait(send_sem, 1))
    mate_copy.wait_send()
    pltpu.make_async_copy(parts_all, parts_all, part_sem.at[0]).wait()


def shards(n, prefill_query, prefill_latent, decode_query, cache, lengths, page_table):
    span, head_here, width = prefill_query.shape
    rows = prefill_latent.shape[0]
    heads = decode_query.shape[1]
    cache_dev = cache.shape[1]
    if head_here != 1 or n % 32 or rows * n != span or span % 512:
        raise ValueError("unexpected sizes")
    line = n // 8
    vmem = pl.BlockSpec(memory_space=pltpu.VMEM)
    anywhere = pl.BlockSpec(memory_space=pl.ANY)
    dma = pltpu.SemaphoreType.DMA
    prefill_out, decode_out = pl.pallas_call(
        functools.partial(kernel, n),
        out_shape=(
            pltpu.VMEM((span, D_LAT), jnp.bfloat16),
            pltpu.VMEM((REQ, D_LAT), jnp.bfloat16),
        ),
        in_specs=[anywhere] * 6,
        out_specs=(vmem, vmem),
        scratch_shapes=[
            pltpu.VMEM((n, rows, width), jnp.bfloat16),
            pltpu.VMEM((REQ, heads, width), jnp.bfloat16),
            pltpu.VMEM((width, span), jnp.bfloat16),
            pltpu.VMEM((span, width), jnp.bfloat16),
            pltpu.VMEM((REQ, width, cache_dev), jnp.bfloat16),
            pltpu.SMEM(lengths.shape, jnp.int32),
            pltpu.SMEM(page_table.shape[::-1], jnp.int32),
            pltpu.VMEM((n // 2, 2, 1, REQ * MSG), jnp.float32),
            pltpu.VMEM((n // 2, 1, REQ * MSG), jnp.float32),
            pltpu.VMEM((n // 2, 1, REQ * MSG), jnp.float32),
            pltpu.VMEM((n // 2, 1, REQ * MSG), jnp.float32),
            dma((6,)),
            dma,
            dma((line,)),
            dma((line,)),
            dma((line,)),
            dma((line,)),
            dma((2,)),
            dma((2,)),
            pltpu.SemaphoreType.REGULAR((line,)),
            pltpu.SemaphoreType.REGULAR((4,)),
            pltpu.SemaphoreType.REGULAR,
        ],
        compiler_params=pltpu.CompilerParams(collective_id=0, has_side_effects=True),
    )(
        prefill_query[:, 0, :].T,
        prefill_latent,
        decode_query,
        jnp.swapaxes(cache, 1, 2),
        lengths,
        page_table.T,
    )
    return prefill_out[:, None, :], decode_out[:, None, :]


def solution(mesh):
    in_specs = (
        P("groups", "ctx", None),
        P(("groups", "ctx"), None),
        P("groups", None, None),
        P("groups", "ctx", None),
        P("groups"),
        P("groups", None),
    )
    out_specs = (P("groups", "ctx", None), P("groups", "ctx", None))
    return jax.shard_map(
        functools.partial(shards, mesh.shape["ctx"]),
        mesh=mesh,
        in_specs=in_specs,
        out_specs=out_specs,
        check_vma=False,
    )
```

```python
import functools

import jax
import jax.numpy as jnp
from jax import lax
from jax.experimental import pallas as pl
from jax.experimental.pallas import tpu as pltpu
from jax.sharding import PartitionSpec as P

D_LAT = 512
PAGE = 16
POOL = 16
REQ = 2

SCALE = 192.0 ** (-0.5)
NEG = -1e30
MSG = D_LAT + 128
NT = (((1,), (1,)), ((), ()))


def kernel(
    n,
    qt_hbm,
    lat_hbm,
    dq_hbm,
    ct_hbm,
    len_hbm,
    pt_hbm,
    pout_ref,
    dout_ref,
    held,
    dq_ref,
    qt,
    q,
    ct,
    len_ref,
    pt_ref,
    parts,
    mate,
    joined,
    moved,
    local_sem,
    send_sem,
    column_sem,
    plane_sem,
    diag_sem,
    pair_sem,
    part_sem,
    mate_sem,
    ready_sem,
    near_sem,
    reach_sem,
):
    me = lax.axis_index("ctx")
    line = n // 8
    core = me % 2
    x = (me // 2) % 2
    y = (me // 4) % 2
    z = me // 8
    far_x, far_y = 1 - x, 1 - y
    rows = lat_hbm.shape[0]
    heads = dq_ref.shape[1]
    chips = n // 2
    chip = me // 2
    span = qt.shape[1]
    cache_dev = ct.shape[2]
    split = rows // 2 if rows % 32 == 0 else rows

    def block(bz, by, bx, bc):
        return ((bz * 2 + by) * 2 + bx) * 2 + bc

    x_peer = block(z, y, far_x, core)
    y_peer = block(z, far_y, x, core)
    pair = block(z, y, x, 1 - core)

    def local(index, source, target):
        copy = pltpu.make_async_copy(source, target, local_sem.at[index])
        copy.start()
        return copy

    own_copy = local(0, lat_hbm, held.at[me])

    barrier = pltpu.get_barrier_semaphore()
    peers = ((x, x_peer), (y, y_peer), (core, pair))
    for side, target in peers:

        @pl.when(side == 0)
        def _(target=target):
            pl.semaphore_signal(barrier, inc=1, device_id={"ctx": target})

    def greet(bz, carry):
        pl.semaphore_signal(barrier, inc=1, device_id={"ctx": block(bz, y, x, core)})
        return carry

    lax.fori_loop(z + 1, line, greet, 0)


    def both(distance, act):
        if distance == 0:
            act(z)
            return
        pl.when(z + distance < line)(lambda: act(z + distance))
        pl.when(z >= distance)(lambda: act(z - distance))

    def move(index, recv, target, part=None):
        ref = held.at[index]
        if part == 0:
            ref = held.at[index, pl.ds(0, split)]
        if part == 1:
            ref = held.at[index, pl.ds(split, rows - split)]
        pltpu.make_async_remote_copy(
            src_ref=ref, dst_ref=ref, send_sem=send_sem, recv_sem=recv, device_id={"ctx": target}
        ).start()

    def blocks_wait(sem, count):
        ref = held.at[pl.ds(0, count)]
        pltpu.make_async_copy(ref, ref, sem).wait()

    def to_pair(bz, by, bx):
        index = block(bz, by, bx, core)
        move(index, pair_sem.at[bz], pair)

    def spread(bz, straight):
        index = block(bz, y, x, core)
        move(index, plane_sem.at[bz], x_peer)
        move(index, plane_sem.at[bz], y_peer)
        if straight:
            move(index, diag_sem.at[bz], block(z, far_y, far_x, core))
        to_pair(bz, y, x)

    def column_step(bz, straight):
        blocks_wait(column_sem.at[bz], 1)
        spread(bz, straight)

    def relay_y(bz):
        if split < rows:
            move(block(bz, y, far_x, core), diag_sem.at[bz], y_peer, 1)

    def relay_x(bz):
        move(block(bz, far_y, x, core), diag_sem.at[bz], x_peer, 0)

    def plane_step(bz, straight=False):
        blocks_wait(plane_sem.at[bz], 2)
        if not straight:
            relay_y(bz)
            relay_x(bz)
        to_pair(bz, y, far_x)
        to_pair(bz, far_y, x)

    def diag_step(bz):
        blocks_wait(diag_sem.at[bz], 1)
        to_pair(bz, far_y, far_x)

    def up_step(distance):
        @pl.when(z + distance < line)
        def _():
            pl.semaphore_wait(ready_sem.at[z + distance], 1)
            own(column_sem.at[z], block(z + distance, y, x, core))

    def own(recv, target):
        pltpu.make_async_remote_copy(
            src_ref=lat_hbm,
            dst_ref=held.at[me],
            send_sem=send_sem,
            recv_sem=recv,
            device_id={"ctx": target},
        ).start()

    def down(bz, carry):
        own(column_sem.at[z], block(bz, y, x, core))
        return carry

    def ready(bz, carry):
        pl.semaphore_signal(ready_sem.at[z], inc=1, device_id={"ctx": block(bz, y, x, core)})
        return carry

    def reach(target, carry):
        pl.semaphore_signal(reach_sem, inc=1, device_id={"ctx": target * 2 + core})
        return carry

    entered = z + x + y + core
    pl.when(entered > 0)(lambda: pl.semaphore_wait(barrier, entered))
    lax.fori_loop(0, z, down, 0)

    plane_sems = (plane_sem, plane_sem, pair_sem)
    for step, (side, target) in enumerate(peers):

        @pl.when(side == 1)
        def _(target=target, step=step):
            pl.semaphore_signal(near_sem.at[step], inc=1, device_id={"ctx": target})
            own(plane_sems[step].at[z], target)

    lax.fori_loop(0, z, ready, 0)
    d_copy = local(2, dq_hbm, dq_ref)
    len_copy = local(3, len_hbm, len_ref)
    pt_copy = local(4, pt_hbm, pt_ref)
    c_copy = local(1, ct_hbm, ct)
    q_copy = local(5, qt_hbm, qt)
    for step, (side, target) in enumerate(peers):

        @pl.when(side == 0)
        def _(target=target, step=step):
            pl.semaphore_wait(near_sem.at[step], 1)
            own(plane_sems[step].at[z], target)
            if step == 0:
                pl.semaphore_signal(near_sem.at[0], inc=1, device_id={"ctx": target})

    own_copy.wait()
    c_copy.wait()
    d_copy.wait()
    len_copy.wait()
    pt_copy.wait()
    latent = held[me]
    row_page = (me * rows + lax.broadcasted_iota(jnp.int32, (1, rows), 1)) // PAGE
    first_page = me * rows // PAGE
    request_of = jnp.zeros((1, rows), jnp.int32)
    for p in range(max(1, rows // PAGE)):
        page = first_page + p
        request = (pt_ref[0, page] * POOL + pt_ref[1, page]) % REQ
        request_of = jnp.where(row_page == page, request, request_of)
    positions = me * cache_dev + lax.broadcasted_iota(jnp.int32, (1, cache_dev), 1)
    for r in range(REQ):
        queries = dq_ref[r]
        keys = ct[r]
        scores = jnp.dot(queries, keys, preferred_element_type=jnp.float32) * SCALE
        page_scores = (
            lax.dot_general(queries, latent, NT, preferred_element_type=jnp.float32) * SCALE
        )
        ok = positions < len_ref[r]
        page_ok = request_of == r
        scores = jnp.where(ok, scores, NEG)
        page_scores = jnp.where(page_ok, page_scores, NEG)
        top = jnp.maximum(
            jnp.max(scores, axis=1, keepdims=True), jnp.max(page_scores, axis=1, keepdims=True)
        )
        weights = jnp.where(ok, jnp.exp(scores - top), 0.0)
        page_weights = jnp.where(page_ok, jnp.exp(page_scores - top), 0.0)
        total = jnp.sum(weights, axis=1, keepdims=True) + jnp.sum(
            page_weights, axis=1, keepdims=True
        )
        mixed = lax.dot_general(
            weights.astype(jnp.bfloat16), keys[:D_LAT], NT, preferred_element_type=jnp.float32
        ) + jnp.dot(
            page_weights.astype(jnp.bfloat16),
            latent[:, :D_LAT],
            preferred_element_type=jnp.float32,
        )
        lane = lax.broadcasted_iota(jnp.int32, (heads, 128), 1)
        tail = jnp.where(lane < 64, top, total)
        parts[:, :, :, r * MSG : r * MSG + D_LAT] = mixed.reshape(chips, 2, 1, D_LAT)
        parts[:, :, :, r * MSG + D_LAT : (r + 1) * MSG] = tail.reshape(chips, 2, 1, 128)

    mate_copy = pltpu.make_async_remote_copy(
        src_ref=parts.at[:, 1 - core],
        dst_ref=mate,
        send_sem=mate_sem.at[0],
        recv_sem=mate_sem.at[1],
        device_id={"ctx": pair},
    )
    mate_copy.start()

    @pl.when(x == 1)
    def _():
        pl.semaphore_wait(near_sem.at[0], 1)

    pl.semaphore_signal(near_sem.at[3], inc=1, device_id={"ctx": y_peer})

    def part_copy(target):
        return pltpu.make_async_remote_copy(
            src_ref=joined.at[target],
            dst_ref=moved.at[chip],
            send_sem=part_sem.at[0],
            recv_sem=part_sem.at[1],
            device_id={"ctx": target * 2 + core},
        )

    def send_part(target, carry):
        part_copy(target).start()
        return carry

    def join():
        mate_copy.wait_recv()
        for r in range(REQ):
            mine = parts[:, core, :, r * MSG : (r + 1) * MSG].reshape(chips, MSG)
            other = mate[:, :, r * MSG : (r + 1) * MSG].reshape(chips, MSG)
            top_mine = mine[:, D_LAT : D_LAT + 1]
            top_other = other[:, D_LAT : D_LAT + 1]
            top = jnp.maximum(top_mine, top_other)
            sum_both = mine * jnp.exp(top_mine - top) + other * jnp.exp(top_other - top)
            lane = lax.broadcasted_iota(jnp.int32, (chips, 128), 1)
            tail = jnp.where(lane < 64, top, sum_both[:, D_LAT:])
            joined[:, :, r * MSG : r * MSG + D_LAT] = sum_both[:, :D_LAT].reshape(chips, 1, D_LAT)
            joined[:, :, r * MSG + D_LAT : (r + 1) * MSG] = tail.reshape(chips, 1, 128)
        moved[chip] = joined[chip]

    quarter = span // 4
    group = n // 4

    def attend(i, first, last):
        start, count = i * quarter, (last - first) * quarter
        keys = held[first * group : last * group].reshape(count, held.shape[2])
        scores = lax.dot_general(
            q[start : start + quarter], keys, NT, preferred_element_type=jnp.float32
        )
        if last == i + 1:
            row = start + lax.broadcasted_iota(jnp.int32, (quarter, count), 0)
            col = first * quarter + lax.broadcasted_iota(jnp.int32, (quarter, count), 1)
            scores = jnp.where(col <= row, scores, NEG)
        top = jnp.max(scores, axis=1, keepdims=True)
        weights = jnp.exp((scores - top) * SCALE)
        total = jnp.sum(weights, axis=1, keepdims=True)
        mixed = jnp.dot(
            weights.astype(jnp.bfloat16), keys[:, :D_LAT], preferred_element_type=jnp.float32
        )
        return top, total, mixed

    def finish(i, total, mixed):
        pout_ref[i * quarter : (i + 1) * quarter, :] = (mixed / total).astype(jnp.bfloat16)

    def await_group(p):
        for bz in range(p * (line // 4), (p + 1) * (line // 4)):
            blocks_wait(pair_sem.at[bz], 4)

    def up_all(first):
        for step in range(first, line):
            up_step(step)

    def transpose_queries():
        q_copy.wait()
        for start in range(0, span, 128):
            q[start : start + 128, :] = qt[:, start : start + 128].T

    pl.when(z > 0)(lambda: up_all(1))
    transpose_queries()
    @pl.when(z == 0)
    def _():
        up_step(1)
        column_step(1, False)
        plane_step(0)
        up_step(2)

    join()

    @pl.when(z > 0)
    def _():
        pl.semaphore_wait(near_sem.at[3], 1)
        lax.fori_loop(0, 4 * z, send_part, 0)
        lax.fori_loop(0, 4 * z, reach, 0)

    pl.when(z == 0)(lambda: pl.semaphore_wait(near_sem.at[3], 1))
    pl.when(z == 0)(lambda: up_all(3))
    for step in range(1, line):
        if step == 1:
            pl.when((z > 0) & (z + 1 < line))(lambda: column_step(z + 1, False))
            pl.when(z > 0)(lambda: column_step(z - 1, False))
            pl.when(z > 0)(lambda: plane_step(z))
        else:
            both(step, lambda bz: column_step(bz, True))
    both(1, lambda bz: plane_step(bz, False))
    pl.when(z < line - 1)(lambda: pl.semaphore_wait(reach_sem, 4 * (line - 1 - z)))
    lax.fori_loop(4 * z, chip, send_part, 0)
    lax.fori_loop(chip + 1, chips, send_part, 0)
    diag_step(z)
    for step in range(2, line - 1):
        both(step, lambda bz: plane_step(bz, True))
    pl.when(z == 0)(lambda: plane_step(line - 1, True))
    pl.when(z == line - 1)(lambda: plane_step(0, True))
    for step in range(1, line):
        both(step, diag_step)

    for p in range(4):
        await_group(p)
    parts_all = moved.at[pl.ds(0, chips - 1)]
    pltpu.make_async_copy(parts_all, parts_all, part_sem.at[1]).wait()
    for r in range(REQ):
        piece = moved[:, :, r * MSG : (r + 1) * MSG].reshape(chips, MSG)
        best = piece[:, D_LAT : D_LAT + 1]
        mass = piece[:, D_LAT + 64 : D_LAT + 65]
        factor = jnp.exp(best - jnp.max(best, axis=0, keepdims=True))
        own_sum = jnp.sum(mass * factor, axis=0, keepdims=True)
        own_out = jnp.sum(piece[:, :D_LAT] * factor, axis=0, keepdims=True)
        dout_ref[r : r + 1, :] = (own_out / own_sum).astype(jnp.bfloat16)

    for i in range(4):
        _, total, mixed = attend(i, 0, i + 1)
        finish(i, total, mixed)

    blocks_wait(send_sem, n - 2)
    blocks_wait(send_sem, 1)
    mate_copy.wait_send()
    pltpu.make_async_copy(parts_all, parts_all, part_sem.at[0]).wait()


def shards(n, prefill_query, prefill_latent, decode_query, cache, lengths, page_table):
    span, head_here, width = prefill_query.shape
    rows = prefill_latent.shape[0]
    heads = decode_query.shape[1]
    cache_dev = cache.shape[1]
    if head_here != 1 or n % 32 or rows * n != span or span % 512:
        raise ValueError("unexpected sizes")
    line = n // 8
    vmem = pl.BlockSpec(memory_space=pltpu.VMEM)
    anywhere = pl.BlockSpec(memory_space=pl.ANY)
    dma = pltpu.SemaphoreType.DMA
    prefill_out, decode_out = pl.pallas_call(
        functools.partial(kernel, n),
        out_shape=(
            pltpu.VMEM((span, D_LAT), jnp.bfloat16),
            pltpu.VMEM((REQ, D_LAT), jnp.bfloat16),
        ),
        in_specs=[anywhere] * 6,
        out_specs=(vmem, vmem),
        scratch_shapes=[
            pltpu.VMEM((n, rows, width), jnp.bfloat16),
            pltpu.VMEM((REQ, heads, width), jnp.bfloat16),
            pltpu.VMEM((width, span), jnp.bfloat16),
            pltpu.VMEM((span, width), jnp.bfloat16),
            pltpu.VMEM((REQ, width, cache_dev), jnp.bfloat16),
            pltpu.SMEM(lengths.shape, jnp.int32),
            pltpu.SMEM(page_table.shape[::-1], jnp.int32),
            pltpu.VMEM((n // 2, 2, 1, REQ * MSG), jnp.float32),
            pltpu.VMEM((n // 2, 1, REQ * MSG), jnp.float32),
            pltpu.VMEM((n // 2, 1, REQ * MSG), jnp.float32),
            pltpu.VMEM((n // 2, 1, REQ * MSG), jnp.float32),
            dma((6,)),
            dma,
            dma((line,)),
            dma((line,)),
            dma((line,)),
            dma((line,)),
            dma((2,)),
            dma((2,)),
            pltpu.SemaphoreType.REGULAR((line,)),
            pltpu.SemaphoreType.REGULAR((4,)),
            pltpu.SemaphoreType.REGULAR,
        ],
        compiler_params=pltpu.CompilerParams(collective_id=0, has_side_effects=True),
    )(
        prefill_query[:, 0, :].T,
        prefill_latent,
        decode_query,
        jnp.swapaxes(cache, 1, 2),
        lengths,
        page_table.T,
    )
    return prefill_out[:, None, :], decode_out[:, None, :]


def solution(mesh):
    in_specs = (
        P("groups", "ctx", None),
        P(("groups", "ctx"), None),
        P("groups", None, None),
        P("groups", "ctx", None),
        P("groups"),
        P("groups", None),
    )
    out_specs = (P("groups", "ctx", None), P("groups", "ctx", None))
    return jax.shard_map(
        functools.partial(shards, mesh.shape["ctx"]),
        mesh=mesh,
        in_specs=in_specs,
        out_specs=out_specs,
        check_vma=False,
    )
```

```python
import functools

import jax
import jax.numpy as jnp
from jax import lax
from jax.experimental import pallas as pl
from jax.experimental.pallas import tpu as pltpu
from jax.sharding import PartitionSpec as P

D_LAT = 512
PAGE = 16
POOL = 16
REQ = 2

SCALE = 192.0 ** (-0.5)
NEG = -1e30
MSG = D_LAT + 128
NT = (((1,), (1,)), ((), ()))


def kernel(
    n,
    qt_hbm,
    lat_hbm,
    dq_hbm,
    ct_hbm,
    len_hbm,
    pt_hbm,
    pout_ref,
    dout_ref,
    held,
    dq_ref,
    qt,
    q,
    ct,
    len_ref,
    pt_ref,
    parts,
    mate,
    joined,
    moved,
    local_sem,
    send_sem,
    column_sem,
    plane_sem,
    diag_sem,
    pair_sem,
    part_sem,
    mate_sem,
    ready_sem,
    near_sem,
    reach_sem,
):
    me = lax.axis_index("ctx")
    line = n // 8
    core = me % 2
    x = (me // 2) % 2
    y = (me // 4) % 2
    z = me // 8
    far_x, far_y = 1 - x, 1 - y
    rows = lat_hbm.shape[0]
    heads = dq_ref.shape[1]
    chips = n // 2
    chip = me // 2
    span = qt.shape[1]
    cache_dev = ct.shape[2]
    split = rows // 2 if rows % 32 == 0 else rows

    def block(bz, by, bx, bc):
        return ((bz * 2 + by) * 2 + bx) * 2 + bc

    x_peer = block(z, y, far_x, core)
    y_peer = block(z, far_y, x, core)
    pair = block(z, y, x, 1 - core)

    def local(index, source, target):
        copy = pltpu.make_async_copy(source, target, local_sem.at[index])
        copy.start()
        return copy

    own_copy = local(0, lat_hbm, held.at[me])

    barrier = pltpu.get_barrier_semaphore()
    peers = ((x, x_peer), (y, y_peer), (core, pair))
    for side, target in peers:

        @pl.when(side == 0)
        def _(target=target):
            pl.semaphore_signal(barrier, inc=1, device_id={"ctx": target})

    def greet(bz, carry):
        pl.semaphore_signal(barrier, inc=1, device_id={"ctx": block(bz, y, x, core)})
        return carry

    lax.fori_loop(z + 1, line, greet, 0)


    def both(distance, act):
        if distance == 0:
            act(z)
            return
        pl.when(z + distance < line)(lambda: act(z + distance))
        pl.when(z >= distance)(lambda: act(z - distance))

    def move(index, recv, target, part=None):
        ref = held.at[index]
        if part == 0:
            ref = held.at[index, pl.ds(0, split)]
        if part == 1:
            ref = held.at[index, pl.ds(split, rows - split)]
        pltpu.make_async_remote_copy(
            src_ref=ref, dst_ref=ref, send_sem=send_sem, recv_sem=recv, device_id={"ctx": target}
        ).start()

    def blocks_wait(sem, count):
        ref = held.at[pl.ds(0, count)]
        pltpu.make_async_copy(ref, ref, sem).wait()

    def to_pair(bz, by, bx):
        index = block(bz, by, bx, core)
        move(index, pair_sem.at[bz], pair)

    def spread(bz, straight):
        index = block(bz, y, x, core)
        move(index, plane_sem.at[bz], x_peer)
        move(index, plane_sem.at[bz], y_peer)
        if straight:
            move(index, diag_sem.at[bz], block(z, far_y, far_x, core))
        to_pair(bz, y, x)

    def column_step(bz, straight):
        blocks_wait(column_sem.at[bz], 1)
        spread(bz, straight)

    def relay_y(bz):
        if split < rows:
            move(block(bz, y, far_x, core), diag_sem.at[bz], y_peer, 1)

    def relay_x(bz):
        move(block(bz, far_y, x, core), diag_sem.at[bz], x_peer, 0)

    def plane_step(bz, straight=False):
        blocks_wait(plane_sem.at[bz], 2)
        if not straight:
            relay_y(bz)
            relay_x(bz)
        to_pair(bz, y, far_x)
        to_pair(bz, far_y, x)

    def diag_step(bz):
        blocks_wait(diag_sem.at[bz], 1)
        to_pair(bz, far_y, far_x)

    def up_step(distance):
        @pl.when(z + distance < line)
        def _():
            pl.semaphore_wait(ready_sem.at[z + distance], 1)
            own(column_sem.at[z], block(z + distance, y, x, core))

    def own(recv, target):
        pltpu.make_async_remote_copy(
            src_ref=lat_hbm,
            dst_ref=held.at[me],
            send_sem=send_sem,
            recv_sem=recv,
            device_id={"ctx": target},
        ).start()

    def down(bz, carry):
        own(column_sem.at[z], block(bz, y, x, core))
        return carry

    def ready(bz, carry):
        pl.semaphore_signal(ready_sem.at[z], inc=1, device_id={"ctx": block(bz, y, x, core)})
        return carry

    def reach(target, carry):
        pl.semaphore_signal(reach_sem, inc=1, device_id={"ctx": target * 2 + core})
        return carry

    entered = z + x + y + core
    pl.when(entered > 0)(lambda: pl.semaphore_wait(barrier, entered))
    lax.fori_loop(0, z, down, 0)

    plane_sems = (plane_sem, plane_sem, pair_sem)
    for step, (side, target) in enumerate(peers):

        @pl.when(side == 1)
        def _(target=target, step=step):
            pl.semaphore_signal(near_sem.at[step], inc=1, device_id={"ctx": target})
            own(plane_sems[step].at[z], target)

    lax.fori_loop(0, z, ready, 0)
    d_copy = local(2, dq_hbm, dq_ref)
    len_copy = local(3, len_hbm, len_ref)
    pt_copy = local(4, pt_hbm, pt_ref)
    c_copy = local(1, ct_hbm, ct)
    q_copy = local(5, qt_hbm, qt)
    for step, (side, target) in enumerate(peers):

        @pl.when(side == 0)
        def _(target=target, step=step):
            pl.semaphore_wait(near_sem.at[step], 1)
            own(plane_sems[step].at[z], target)
            if step == 0:
                pl.semaphore_signal(near_sem.at[0], inc=1, device_id={"ctx": target})

    own_copy.wait()
    c_copy.wait()
    d_copy.wait()
    len_copy.wait()
    pt_copy.wait()
    latent = held[me]
    row_page = (me * rows + lax.broadcasted_iota(jnp.int32, (1, rows), 1)) // PAGE
    first_page = me * rows // PAGE
    request_of = jnp.zeros((1, rows), jnp.int32)
    for p in range(max(1, rows // PAGE)):
        page = first_page + p
        request = (pt_ref[0, page] * POOL + pt_ref[1, page]) % REQ
        request_of = jnp.where(row_page == page, request, request_of)
    positions = me * cache_dev + lax.broadcasted_iota(jnp.int32, (1, cache_dev), 1)
    for r in range(REQ):
        queries = dq_ref[r]
        keys = ct[r]
        scores = jnp.dot(queries, keys, preferred_element_type=jnp.float32) * SCALE
        page_scores = (
            lax.dot_general(queries, latent, NT, preferred_element_type=jnp.float32) * SCALE
        )
        ok = positions < len_ref[r]
        page_ok = request_of == r
        scores = jnp.where(ok, scores, NEG)
        page_scores = jnp.where(page_ok, page_scores, NEG)
        top = jnp.maximum(
            jnp.max(scores, axis=1, keepdims=True), jnp.max(page_scores, axis=1, keepdims=True)
        )
        weights = jnp.where(ok, jnp.exp(scores - top), 0.0)
        page_weights = jnp.where(page_ok, jnp.exp(page_scores - top), 0.0)
        total = jnp.sum(weights, axis=1, keepdims=True) + jnp.sum(
            page_weights, axis=1, keepdims=True
        )
        mixed = lax.dot_general(
            weights.astype(jnp.bfloat16), keys[:D_LAT], NT, preferred_element_type=jnp.float32
        ) + jnp.dot(
            page_weights.astype(jnp.bfloat16),
            latent[:, :D_LAT],
            preferred_element_type=jnp.float32,
        )
        lane = lax.broadcasted_iota(jnp.int32, (heads, 128), 1)
        tail = jnp.where(lane < 64, top, total)
        parts[:, :, :, r * MSG : r * MSG + D_LAT] = mixed.reshape(chips, 2, 1, D_LAT)
        parts[:, :, :, r * MSG + D_LAT : (r + 1) * MSG] = tail.reshape(chips, 2, 1, 128)

    mate_copy = pltpu.make_async_remote_copy(
        src_ref=parts.at[:, 1 - core],
        dst_ref=mate,
        send_sem=mate_sem.at[0],
        recv_sem=mate_sem.at[1],
        device_id={"ctx": pair},
    )
    mate_copy.start()

    @pl.when(x == 1)
    def _():
        pl.semaphore_wait(near_sem.at[0], 1)

    pl.semaphore_signal(near_sem.at[3], inc=1, device_id={"ctx": y_peer})

    def part_copy(target):
        return pltpu.make_async_remote_copy(
            src_ref=joined.at[target],
            dst_ref=moved.at[chip],
            send_sem=part_sem.at[0],
            recv_sem=part_sem.at[1],
            device_id={"ctx": target * 2 + core},
        )

    def send_part(target, carry):
        part_copy(target).start()
        return carry

    def join():
        mate_copy.wait_recv()
        for r in range(REQ):
            mine = parts[:, core, :, r * MSG : (r + 1) * MSG].reshape(chips, MSG)
            other = mate[:, :, r * MSG : (r + 1) * MSG].reshape(chips, MSG)
            top_mine = mine[:, D_LAT : D_LAT + 1]
            top_other = other[:, D_LAT : D_LAT + 1]
            top = jnp.maximum(top_mine, top_other)
            sum_both = mine * jnp.exp(top_mine - top) + other * jnp.exp(top_other - top)
            lane = lax.broadcasted_iota(jnp.int32, (chips, 128), 1)
            tail = jnp.where(lane < 64, top, sum_both[:, D_LAT:])
            joined[:, :, r * MSG : r * MSG + D_LAT] = sum_both[:, :D_LAT].reshape(chips, 1, D_LAT)
            joined[:, :, r * MSG + D_LAT : (r + 1) * MSG] = tail.reshape(chips, 1, 128)
        moved[chip] = joined[chip]

    quarter = span // 4
    group = n // 4

    def score(i):
        start, stop = i * quarter, (i + 1) * quarter
        keys = held[: (i + 1) * group].reshape(stop, held.shape[2])
        scores = lax.dot_general(
            q[start:stop], keys, NT, preferred_element_type=jnp.float32
        )
        row = lax.broadcasted_iota(jnp.int32, (quarter, quarter), 0)
        col = lax.broadcasted_iota(jnp.int32, (quarter, quarter), 1)
        last = jnp.where(col <= row, scores[:, start:], NEG)
        if i:
            last = jnp.concatenate([scores[:, :start], last], axis=1)
        return i, keys, last

    def weigh(i, keys, scores):
        top = jnp.max(scores, axis=1, keepdims=True)
        weights = jnp.exp((scores - top) * SCALE)
        total = jnp.sum(weights, axis=1, keepdims=True)
        mixed = jnp.dot(
            weights.astype(jnp.bfloat16), keys[:, :D_LAT], preferred_element_type=jnp.float32
        )
        pout_ref[i * quarter : (i + 1) * quarter, :] = (mixed / total).astype(jnp.bfloat16)

    def await_group(p):
        for bz in range(p * (line // 4), (p + 1) * (line // 4)):
            blocks_wait(pair_sem.at[bz], 4)

    def up_all(first):
        for step in range(first, line):
            up_step(step)

    def transpose_queries():
        q_copy.wait()
        for start in range(0, span, 128):
            q[start : start + 128, :] = qt[:, start : start + 128].T

    pl.when(z > 0)(lambda: up_all(1))
    transpose_queries()
    @pl.when(z == 0)
    def _():
        up_step(1)
        column_step(1, False)
        plane_step(0)
        up_step(2)

    join()

    @pl.when(z > 0)
    def _():
        pl.semaphore_wait(near_sem.at[3], 1)
        lax.fori_loop(0, 4 * z, send_part, 0)
        lax.fori_loop(0, 4 * z, reach, 0)

    pl.when(z == 0)(lambda: pl.semaphore_wait(near_sem.at[3], 1))
    pl.when(z == 0)(lambda: up_all(3))
    for step in range(1, line):
        if step == 1:
            pl.when((z > 0) & (z + 1 < line))(lambda: column_step(z + 1, False))
            pl.when(z > 0)(lambda: column_step(z - 1, False))
            pl.when(z > 0)(lambda: plane_step(z))
        else:
            both(step, lambda bz: column_step(bz, True))
    both(1, lambda bz: plane_step(bz, False))
    pl.when(z < line - 1)(lambda: pl.semaphore_wait(reach_sem, 4 * (line - 1 - z)))
    lax.fori_loop(4 * z, chip, send_part, 0)
    lax.fori_loop(chip + 1, chips, send_part, 0)
    diag_step(z)
    for step in range(2, line - 1):
        both(step, lambda bz: plane_step(bz, True))
    pl.when(z == 0)(lambda: plane_step(line - 1, True))
    pl.when(z == line - 1)(lambda: plane_step(0, True))
    for step in range(1, line):
        both(step, diag_step)

    for p in range(4):
        await_group(p)
    parts_all = moved.at[pl.ds(0, chips - 1)]
    pltpu.make_async_copy(parts_all, parts_all, part_sem.at[1]).wait()
    for r in range(REQ):
        piece = moved[:, :, r * MSG : (r + 1) * MSG].reshape(chips, MSG)
        best = piece[:, D_LAT : D_LAT + 1]
        mass = piece[:, D_LAT + 64 : D_LAT + 65]
        factor = jnp.exp(best - jnp.max(best, axis=0, keepdims=True))
        own_sum = jnp.sum(mass * factor, axis=0, keepdims=True)
        own_out = jnp.sum(piece[:, :D_LAT] * factor, axis=0, keepdims=True)
        dout_ref[r : r + 1, :] = (own_out / own_sum).astype(jnp.bfloat16)

    scored = score(0)
    for i in range(1, 4):
        after = score(i)
        weigh(*scored)
        scored = after
    weigh(*scored)

    blocks_wait(send_sem, n - 2)
    blocks_wait(send_sem, 1)
    mate_copy.wait_send()
    pltpu.make_async_copy(parts_all, parts_all, part_sem.at[0]).wait()


def shards(n, prefill_query, prefill_latent, decode_query, cache, lengths, page_table):
    span, head_here, width = prefill_query.shape
    rows = prefill_latent.shape[0]
    heads = decode_query.shape[1]
    cache_dev = cache.shape[1]
    if head_here != 1 or n % 32 or rows * n != span or span % 512:
        raise ValueError("unexpected sizes")
    line = n // 8
    vmem = pl.BlockSpec(memory_space=pltpu.VMEM)
    anywhere = pl.BlockSpec(memory_space=pl.ANY)
    dma = pltpu.SemaphoreType.DMA
    prefill_out, decode_out = pl.pallas_call(
        functools.partial(kernel, n),
        out_shape=(
            pltpu.VMEM((span, D_LAT), jnp.bfloat16),
            pltpu.VMEM((REQ, D_LAT), jnp.bfloat16),
        ),
        in_specs=[anywhere] * 6,
        out_specs=(vmem, vmem),
        scratch_shapes=[
            pltpu.VMEM((n, rows, width), jnp.bfloat16),
            pltpu.VMEM((REQ, heads, width), jnp.bfloat16),
            pltpu.VMEM((width, span), jnp.bfloat16),
            pltpu.VMEM((span, width), jnp.bfloat16),
            pltpu.VMEM((REQ, width, cache_dev), jnp.bfloat16),
            pltpu.SMEM(lengths.shape, jnp.int32),
            pltpu.SMEM(page_table.shape[::-1], jnp.int32),
            pltpu.VMEM((n // 2, 2, 1, REQ * MSG), jnp.float32),
            pltpu.VMEM((n // 2, 1, REQ * MSG), jnp.float32),
            pltpu.VMEM((n // 2, 1, REQ * MSG), jnp.float32),
            pltpu.VMEM((n // 2, 1, REQ * MSG), jnp.float32),
            dma((6,)),
            dma,
            dma((line,)),
            dma((line,)),
            dma((line,)),
            dma((line,)),
            dma((2,)),
            dma((2,)),
            pltpu.SemaphoreType.REGULAR((line,)),
            pltpu.SemaphoreType.REGULAR((4,)),
            pltpu.SemaphoreType.REGULAR,
        ],
        compiler_params=pltpu.CompilerParams(collective_id=0, has_side_effects=True),
    )(
        prefill_query[:, 0, :].T,
        prefill_latent,
        decode_query,
        jnp.swapaxes(cache, 1, 2),
        lengths,
        page_table.T,
    )
    return prefill_out[:, None, :], decode_out[:, None, :]


def solution(mesh):
    in_specs = (
        P("groups", "ctx", None),
        P(("groups", "ctx"), None),
        P("groups", None, None),
        P("groups", "ctx", None),
        P("groups"),
        P("groups", None),
    )
    out_specs = (P("groups", "ctx", None), P("groups", "ctx", None))
    return jax.shard_map(
        functools.partial(shards, mesh.shape["ctx"]),
        mesh=mesh,
        in_specs=in_specs,
        out_specs=out_specs,
        check_vma=False,
    )
```

```python
import functools

import jax
import jax.numpy as jnp
from jax import lax
from jax.experimental import pallas as pl
from jax.experimental.pallas import tpu as pltpu
from jax.sharding import PartitionSpec as P

D_LAT = 512
PAGE = 16
POOL = 16
REQ = 2

SCALE = 192.0 ** (-0.5)
NEG = -1e30
MSG = D_LAT + 128
NT = (((1,), (1,)), ((), ()))


def kernel(
    n,
    qt_hbm,
    lat_hbm,
    dq_hbm,
    ct_hbm,
    len_hbm,
    pt_hbm,
    pout_ref,
    dout_ref,
    held,
    dq_ref,
    qt,
    q,
    ct,
    len_ref,
    pt_ref,
    parts,
    mate,
    joined,
    moved,
    acc,
    tops,
    sums,
    local_sem,
    send_sem,
    column_sem,
    plane_sem,
    diag_sem,
    pair_sem,
    part_sem,
    mate_sem,
    ready_sem,
    near_sem,
    reach_sem,
):
    me = lax.axis_index("ctx")
    line = n // 8
    core = me % 2
    x = (me // 2) % 2
    y = (me // 4) % 2
    z = me // 8
    far_x, far_y = 1 - x, 1 - y
    rows = lat_hbm.shape[0]
    heads = dq_ref.shape[1]
    chips = n // 2
    chip = me // 2
    span = qt.shape[1]
    cache_dev = ct.shape[2]
    split = rows // 2 if rows % 32 == 0 else rows

    def block(bz, by, bx, bc):
        return ((bz * 2 + by) * 2 + bx) * 2 + bc

    x_peer = block(z, y, far_x, core)
    y_peer = block(z, far_y, x, core)
    pair = block(z, y, x, 1 - core)

    def local(index, source, target):
        copy = pltpu.make_async_copy(source, target, local_sem.at[index])
        copy.start()
        return copy

    own_copy = local(0, lat_hbm, held.at[chip, core])

    barrier = pltpu.get_barrier_semaphore()
    peers = ((x, x_peer), (y, y_peer), (core, pair))
    for side, target in peers:

        @pl.when(side == 0)
        def _(target=target):
            pl.semaphore_signal(barrier, inc=1, device_id={"ctx": target})

    def greet(bz, carry):
        pl.semaphore_signal(barrier, inc=1, device_id={"ctx": block(bz, y, x, core)})
        return carry

    lax.fori_loop(z + 1, line, greet, 0)


    def both(distance, act):
        if distance == 0:
            act(z)
            return
        pl.when(z + distance < line)(lambda: act(z + distance))
        pl.when(z >= distance)(lambda: act(z - distance))

    def move(index, recv, target, part=None):
        ref = held.at[index // 2, index % 2]
        if part == 0:
            ref = held.at[index // 2, index % 2, pl.ds(0, split)]
        if part == 1:
            ref = held.at[index // 2, index % 2, pl.ds(split, rows - split)]
        pltpu.make_async_remote_copy(
            src_ref=ref, dst_ref=ref, send_sem=send_sem, recv_sem=recv, device_id={"ctx": target}
        ).start()

    def blocks_wait(sem, count):
        ref = held.at[0, 0] if count == 1 else held.at[pl.ds(0, count // 2)]
        pltpu.make_async_copy(ref, ref, sem).wait()

    def to_pair(bz, by, bx):
        index = block(bz, by, bx, core)
        move(index, pair_sem.at[bz], pair)

    def spread(bz, straight):
        index = block(bz, y, x, core)
        move(index, plane_sem.at[bz], x_peer)
        move(index, plane_sem.at[bz], y_peer)
        if straight:
            move(index, diag_sem.at[bz], block(z, far_y, far_x, core))
        to_pair(bz, y, x)

    def column_step(bz, straight):
        blocks_wait(column_sem.at[bz], 1)
        spread(bz, straight)

    def relay_y(bz):
        if split < rows:
            move(block(bz, y, far_x, core), diag_sem.at[bz], y_peer, 1)

    def relay_x(bz):
        move(block(bz, far_y, x, core), diag_sem.at[bz], x_peer, 0)

    def plane_step(bz, straight=False):
        blocks_wait(plane_sem.at[bz], 2)
        if not straight:
            relay_y(bz)
            relay_x(bz)
        to_pair(bz, y, far_x)
        to_pair(bz, far_y, x)

    def diag_step(bz):
        blocks_wait(diag_sem.at[bz], 1)
        to_pair(bz, far_y, far_x)

    def up_step(distance):
        @pl.when(z + distance < line)
        def _():
            pl.semaphore_wait(ready_sem.at[z + distance], 1)
            own(column_sem.at[z], block(z + distance, y, x, core))

    def own(recv, target):
        pltpu.make_async_remote_copy(
            src_ref=lat_hbm,
            dst_ref=held.at[chip, core],
            send_sem=send_sem,
            recv_sem=recv,
            device_id={"ctx": target},
        ).start()

    def down(bz, carry):
        own(column_sem.at[z], block(bz, y, x, core))
        return carry

    def ready(bz, carry):
        pl.semaphore_signal(ready_sem.at[z], inc=1, device_id={"ctx": block(bz, y, x, core)})
        return carry

    def reach(target, carry):
        pl.semaphore_signal(reach_sem, inc=1, device_id={"ctx": target * 2 + core})
        return carry

    entered = z + x + y + core
    pl.when(entered > 0)(lambda: pl.semaphore_wait(barrier, entered))
    lax.fori_loop(0, z, down, 0)

    plane_sems = (plane_sem, plane_sem, pair_sem)
    for step, (side, target) in enumerate(peers):

        @pl.when(side == 1)
        def _(target=target, step=step):
            pl.semaphore_signal(near_sem.at[step], inc=1, device_id={"ctx": target})
            own(plane_sems[step].at[z], target)

    lax.fori_loop(0, z, ready, 0)
    d_copy = local(2, dq_hbm, dq_ref)
    len_copy = local(3, len_hbm, len_ref)
    pt_copy = local(4, pt_hbm, pt_ref)
    c_copy = local(1, ct_hbm, ct)
    q_copy = local(5, qt_hbm, qt)
    for step, (side, target) in enumerate(peers):

        @pl.when(side == 0)
        def _(target=target, step=step):
            pl.semaphore_wait(near_sem.at[step], 1)
            own(plane_sems[step].at[z], target)
            if step == 0:
                pl.semaphore_signal(near_sem.at[0], inc=1, device_id={"ctx": target})

    own_copy.wait()
    c_copy.wait()
    d_copy.wait()
    len_copy.wait()
    pt_copy.wait()
    latent = held[chip, core]
    row_page = (me * rows + lax.broadcasted_iota(jnp.int32, (1, rows), 1)) // PAGE
    first_page = me * rows // PAGE
    request_of = jnp.zeros((1, rows), jnp.int32)
    for p in range(max(1, rows // PAGE)):
        page = first_page + p
        request = (pt_ref[0, page] * POOL + pt_ref[1, page]) % REQ
        request_of = jnp.where(row_page == page, request, request_of)
    positions = me * cache_dev + lax.broadcasted_iota(jnp.int32, (1, cache_dev), 1)
    for r in range(REQ):
        queries = dq_ref[r]
        keys = ct[r]
        scores = jnp.dot(queries, keys, preferred_element_type=jnp.float32) * SCALE
        page_scores = (
            lax.dot_general(queries, latent, NT, preferred_element_type=jnp.float32) * SCALE
        )
        ok = positions < len_ref[r]
        page_ok = request_of == r
        scores = jnp.where(ok, scores, NEG)
        page_scores = jnp.where(page_ok, page_scores, NEG)
        top = jnp.maximum(
            jnp.max(scores, axis=1, keepdims=True), jnp.max(page_scores, axis=1, keepdims=True)
        )
        weights = jnp.where(ok, jnp.exp(scores - top), 0.0)
        page_weights = jnp.where(page_ok, jnp.exp(page_scores - top), 0.0)
        total = jnp.sum(weights, axis=1, keepdims=True) + jnp.sum(
            page_weights, axis=1, keepdims=True
        )
        mixed = lax.dot_general(
            weights.astype(jnp.bfloat16), keys[:D_LAT], NT, preferred_element_type=jnp.float32
        ) + jnp.dot(
            page_weights.astype(jnp.bfloat16),
            latent[:, :D_LAT],
            preferred_element_type=jnp.float32,
        )
        lane = lax.broadcasted_iota(jnp.int32, (heads, 128), 1)
        tail = jnp.where(lane < 64, top, total)
        parts[:, :, :, r * MSG : r * MSG + D_LAT] = mixed.reshape(chips, 2, 1, D_LAT)
        parts[:, :, :, r * MSG + D_LAT : (r + 1) * MSG] = tail.reshape(chips, 2, 1, 128)

    mate_copy = pltpu.make_async_remote_copy(
        src_ref=parts.at[:, 1 - core],
        dst_ref=mate,
        send_sem=mate_sem.at[0],
        recv_sem=mate_sem.at[1],
        device_id={"ctx": pair},
    )
    mate_copy.start()

    @pl.when(x == 1)
    def _():
        pl.semaphore_wait(near_sem.at[0], 1)

    pl.semaphore_signal(near_sem.at[3], inc=1, device_id={"ctx": y_peer})

    def part_copy(target):
        return pltpu.make_async_remote_copy(
            src_ref=joined.at[target],
            dst_ref=moved.at[chip],
            send_sem=part_sem.at[0],
            recv_sem=part_sem.at[1],
            device_id={"ctx": target * 2 + core},
        )

    def send_part(target, carry):
        part_copy(target).start()
        return carry

    def join():
        mate_copy.wait_recv()
        for r in range(REQ):
            mine = parts[:, core, :, r * MSG : (r + 1) * MSG].reshape(chips, MSG)
            other = mate[:, :, r * MSG : (r + 1) * MSG].reshape(chips, MSG)
            top_mine = mine[:, D_LAT : D_LAT + 1]
            top_other = other[:, D_LAT : D_LAT + 1]
            top = jnp.maximum(top_mine, top_other)
            sum_both = mine * jnp.exp(top_mine - top) + other * jnp.exp(top_other - top)
            lane = lax.broadcasted_iota(jnp.int32, (chips, 128), 1)
            tail = jnp.where(lane < 64, top, sum_both[:, D_LAT:])
            joined[:, :, r * MSG : r * MSG + D_LAT] = sum_both[:, :D_LAT].reshape(chips, 1, D_LAT)
            joined[:, :, r * MSG + D_LAT : (r + 1) * MSG] = tail.reshape(chips, 1, 128)
        moved[chip] = joined[chip]

    quarter = span // 4
    group = n // 4

    def score(i, side=None):
        pairs, before = (i + 1) * group // 2, i * group // 2 * rows
        if side is None:
            keys = held[:pairs].reshape(pairs * 2 * rows, held.shape[3])
            before = before * 2
        else:
            keys = held[:pairs, side].reshape(pairs * rows, held.shape[3])
        scores = lax.dot_general(
            q[i * quarter : (i + 1) * quarter], keys, NT, preferred_element_type=jnp.float32
        )
        fresh = keys.shape[0] - before
        col = lax.broadcasted_iota(jnp.int32, (1, fresh), 1)
        if side is not None:
            col = col + (col // rows + side) * rows
        row = lax.broadcasted_iota(jnp.int32, (quarter, fresh), 0)
        last = jnp.where(col <= row, scores[:, before:], NEG)
        if i:
            last = jnp.concatenate([scores[:, :before], last], axis=1)
        return i, keys, last

    def wide(value, count):
        return jnp.concatenate([value] * (count // 128), axis=1)

    def weigh(i, keys, scores, first, last):
        here = slice(i * quarter, (i + 1) * quarter)
        top = jnp.broadcast_to(jnp.max(scores, axis=1, keepdims=True), (quarter, 128))
        if not first:
            old = tops[here, :]
            top = jnp.maximum(top, old)
            fade = jnp.exp((old - top) * SCALE)
        weights = jnp.exp((scores - wide(top, scores.shape[1])) * SCALE)
        total = jnp.broadcast_to(jnp.sum(weights, axis=1, keepdims=True), (quarter, 128))
        mixed = jnp.dot(
            weights.astype(jnp.bfloat16), keys[:, :D_LAT], preferred_element_type=jnp.float32
        )
        if not first:
            total = total + sums[here, :] * fade
            mixed = mixed + acc[here, :] * wide(fade, D_LAT)
        if last:
            pout_ref[here, :] = (mixed * wide(1.0 / total, D_LAT)).astype(jnp.bfloat16)
        else:
            tops[here, :] = top
            sums[here, :] = total
            acc[here, :] = mixed

    def attend(side, first, last):
        scored = score(0, side)
        for i in range(1, 4):
            after = score(i, side)
            weigh(*scored, first, last)
            scored = after
        weigh(*scored, first, last)

    parts_all = moved.at[pl.ds(0, chips - 1)]

    def decode_finish():
        pltpu.make_async_copy(parts_all, parts_all, part_sem.at[1]).wait()
        for r in range(REQ):
            piece = moved[:, :, r * MSG : (r + 1) * MSG].reshape(chips, MSG)
            best = piece[:, D_LAT : D_LAT + 1]
            mass = piece[:, D_LAT + 64 : D_LAT + 65]
            factor = jnp.exp(best - jnp.max(best, axis=0, keepdims=True))
            own_sum = jnp.sum(mass * factor, axis=0, keepdims=True)
            own_out = jnp.sum(piece[:, :D_LAT] * factor, axis=0, keepdims=True)
            dout_ref[r : r + 1, :] = (own_out / own_sum).astype(jnp.bfloat16)

    def send_parts():
        pl.when(z < line - 1)(lambda: pl.semaphore_wait(reach_sem, 4 * (line - 1 - z)))
        lax.fori_loop(4 * z, chip, send_part, 0)
        lax.fori_loop(chip + 1, chips, send_part, 0)

    def await_group(p):
        for bz in range(p * (line // 4), (p + 1) * (line // 4)):
            blocks_wait(pair_sem.at[bz], 4)

    def up_all(first):
        for step in range(first, line):
            up_step(step)

    def transpose_queries():
        q_copy.wait()
        for start in range(0, span, 128):
            q[start : start + 128, :] = qt[:, start : start + 128].T

    pl.when(z > 0)(lambda: up_all(1))
    transpose_queries()
    @pl.when(z == 0)
    def _():
        up_step(1)
        column_step(1, False)
        plane_step(0)
        up_step(2)

    join()

    @pl.when(z > 0)
    def _():
        pl.semaphore_wait(near_sem.at[3], 1)
        lax.fori_loop(0, 4 * z, send_part, 0)
        lax.fori_loop(0, 4 * z, reach, 0)

    pl.when(z == 0)(lambda: pl.semaphore_wait(near_sem.at[3], 1))
    pl.when(z == 0)(lambda: up_all(3))
    for step in range(1, line):
        if step == 1:
            pl.when((z > 0) & (z + 1 < line))(lambda: column_step(z + 1, False))
            pl.when(z > 0)(lambda: column_step(z - 1, False))
            pl.when(z > 0)(lambda: plane_step(z))
        else:
            both(step, lambda bz: column_step(bz, True))
    both(1, lambda bz: plane_step(bz, False))
    pl.when(core == 0)(send_parts)
    diag_step(z)
    for step in range(2, line - 1):
        both(step, lambda bz: plane_step(bz, True))
    pl.when(z == 0)(lambda: plane_step(line - 1, True))
    pl.when(z == line - 1)(lambda: plane_step(0, True))
    for step in range(1, line):
        both(step, diag_step)

    pl.when(core == 1)(send_parts)
    pl.when(core == 1)(lambda: attend(1, True, False))
    pl.when(core == 1)(decode_finish)
    for p in range(4):
        await_group(p)
    pl.when(core == 0)(lambda: attend(None, True, True))
    pl.when(core == 1)(lambda: attend(0, False, True))

    pl.when(core == 0)(decode_finish)
    blocks_wait(send_sem, n - 2)
    blocks_wait(send_sem, 1)
    mate_copy.wait_send()
    pltpu.make_async_copy(parts_all, parts_all, part_sem.at[0]).wait()


def shards(n, prefill_query, prefill_latent, decode_query, cache, lengths, page_table):
    span, head_here, width = prefill_query.shape
    rows = prefill_latent.shape[0]
    heads = decode_query.shape[1]
    cache_dev = cache.shape[1]
    if head_here != 1 or n % 32 or rows * n != span or span % 512:
        raise ValueError("unexpected sizes")
    line = n // 8
    vmem = pl.BlockSpec(memory_space=pltpu.VMEM)
    anywhere = pl.BlockSpec(memory_space=pl.ANY)
    dma = pltpu.SemaphoreType.DMA
    prefill_out, decode_out = pl.pallas_call(
        functools.partial(kernel, n),
        out_shape=(
            pltpu.VMEM((span, D_LAT), jnp.bfloat16),
            pltpu.VMEM((REQ, D_LAT), jnp.bfloat16),
        ),
        in_specs=[anywhere] * 6,
        out_specs=(vmem, vmem),
        scratch_shapes=[
            pltpu.VMEM((n // 2, 2, rows, width), jnp.bfloat16),
            pltpu.VMEM((REQ, heads, width), jnp.bfloat16),
            pltpu.VMEM((width, span), jnp.bfloat16),
            pltpu.VMEM((span, width), jnp.bfloat16),
            pltpu.VMEM((REQ, width, cache_dev), jnp.bfloat16),
            pltpu.SMEM(lengths.shape, jnp.int32),
            pltpu.SMEM(page_table.shape[::-1], jnp.int32),
            pltpu.VMEM((n // 2, 2, 1, REQ * MSG), jnp.float32),
            pltpu.VMEM((n // 2, 1, REQ * MSG), jnp.float32),
            pltpu.VMEM((n // 2, 1, REQ * MSG), jnp.float32),
            pltpu.VMEM((n // 2, 1, REQ * MSG), jnp.float32),
            pltpu.VMEM((span, D_LAT), jnp.float32),
            pltpu.VMEM((span, 128), jnp.float32),
            pltpu.VMEM((span, 128), jnp.float32),
            dma((6,)),
            dma,
            dma((line,)),
            dma((line,)),
            dma((line,)),
            dma((line,)),
            dma((2,)),
            dma((2,)),
            pltpu.SemaphoreType.REGULAR((line,)),
            pltpu.SemaphoreType.REGULAR((4,)),
            pltpu.SemaphoreType.REGULAR,
        ],
        compiler_params=pltpu.CompilerParams(collective_id=0, has_side_effects=True),
    )(
        prefill_query[:, 0, :].T,
        prefill_latent,
        decode_query,
        jnp.swapaxes(cache, 1, 2),
        lengths,
        page_table.T,
    )
    return prefill_out[:, None, :], decode_out[:, None, :]


def solution(mesh):
    in_specs = (
        P("groups", "ctx", None),
        P(("groups", "ctx"), None),
        P("groups", None, None),
        P("groups", "ctx", None),
        P("groups"),
        P("groups", None),
    )
    out_specs = (P("groups", "ctx", None), P("groups", "ctx", None))
    return jax.shard_map(
        functools.partial(shards, mesh.shape["ctx"]),
        mesh=mesh,
        in_specs=in_specs,
        out_specs=out_specs,
        check_vma=False,
    )
```

```python
import functools

import jax
import jax.numpy as jnp
from jax import lax
from jax.experimental import pallas as pl
from jax.experimental.pallas import tpu as pltpu
from jax.sharding import PartitionSpec as P

D_LAT = 512
PAGE = 16
POOL = 16
REQ = 2

SCALE = 192.0 ** (-0.5)
NEG = -1e30
MSG = D_LAT + 128
NT = (((1,), (1,)), ((), ()))


def kernel(
    n,
    qt_hbm,
    lat_hbm,
    dq_hbm,
    ct_hbm,
    len_hbm,
    pt_hbm,
    pout_ref,
    dout_ref,
    held,
    dq_ref,
    qt,
    q,
    ct,
    len_ref,
    pt_ref,
    parts,
    mate,
    joined,
    moved,
    acc,
    tops,
    sums,
    local_sem,
    send_sem,
    column_sem,
    plane_sem,
    diag_sem,
    pair_sem,
    part_sem,
    mate_sem,
    ready_sem,
    near_sem,
    reach_sem,
):
    me = lax.axis_index("ctx")
    line = n // 8
    core = me % 2
    x = (me // 2) % 2
    y = (me // 4) % 2
    z = me // 8
    far_x, far_y = 1 - x, 1 - y
    rows = lat_hbm.shape[0]
    heads = dq_ref.shape[1]
    chips = n // 2
    chip = me // 2
    span = qt.shape[1]
    cache_dev = ct.shape[2]
    split = rows // 2 if rows % 32 == 0 else rows

    def block(bz, by, bx, bc):
        return ((bz * 2 + by) * 2 + bx) * 2 + bc

    x_peer = block(z, y, far_x, core)
    y_peer = block(z, far_y, x, core)
    pair = block(z, y, x, 1 - core)

    def local(index, source, target):
        copy = pltpu.make_async_copy(source, target, local_sem.at[index])
        copy.start()
        return copy

    own_copy = local(0, lat_hbm, held.at[chip, core])

    barrier = pltpu.get_barrier_semaphore()
    peers = ((x, x_peer), (y, y_peer), (core, pair))
    for side, target in peers:

        @pl.when(side == 0)
        def _(target=target):
            pl.semaphore_signal(barrier, inc=1, device_id={"ctx": target})

    def greet(bz, carry):
        pl.semaphore_signal(barrier, inc=1, device_id={"ctx": block(bz, y, x, core)})
        return carry

    lax.fori_loop(z + 1, line, greet, 0)


    def both(distance, act):
        if distance == 0:
            act(z)
            return
        pl.when(z + distance < line)(lambda: act(z + distance))
        pl.when(z >= distance)(lambda: act(z - distance))

    def move(index, recv, target, part=None):
        ref = held.at[index // 2, index % 2]
        if part == 0:
            ref = held.at[index // 2, index % 2, pl.ds(0, split)]
        if part == 1:
            ref = held.at[index // 2, index % 2, pl.ds(split, rows - split)]
        pltpu.make_async_remote_copy(
            src_ref=ref, dst_ref=ref, send_sem=send_sem, recv_sem=recv, device_id={"ctx": target}
        ).start()

    def blocks_wait(sem, count):
        ref = held.at[0, 0] if count == 1 else held.at[pl.ds(0, count // 2)]
        pltpu.make_async_copy(ref, ref, sem).wait()

    def to_pair(bz, by, bx):
        index = block(bz, by, bx, core)
        move(index, pair_sem.at[bz], pair)

    def spread(bz, straight):
        index = block(bz, y, x, core)
        move(index, plane_sem.at[bz], x_peer)
        move(index, plane_sem.at[bz], y_peer)
        if straight:
            move(index, diag_sem.at[bz], block(z, far_y, far_x, core))
        to_pair(bz, y, x)

    def column_step(bz, straight):
        blocks_wait(column_sem.at[bz], 1)
        spread(bz, straight)

    def relay_y(bz):
        if split < rows:
            move(block(bz, y, far_x, core), diag_sem.at[bz], y_peer, 1)

    def relay_x(bz):
        move(block(bz, far_y, x, core), diag_sem.at[bz], x_peer, 0)

    def plane_step(bz, straight=False):
        blocks_wait(plane_sem.at[bz], 2)
        if not straight:
            relay_y(bz)
            relay_x(bz)
        to_pair(bz, y, far_x)
        to_pair(bz, far_y, x)

    def diag_step(bz):
        blocks_wait(diag_sem.at[bz], 1)
        to_pair(bz, far_y, far_x)

    def up_step(distance):
        @pl.when(z + distance < line)
        def _():
            pl.semaphore_wait(ready_sem.at[z + distance], 1)
            own(column_sem.at[z], block(z + distance, y, x, core))

    def own(recv, target):
        pltpu.make_async_remote_copy(
            src_ref=lat_hbm,
            dst_ref=held.at[chip, core],
            send_sem=send_sem,
            recv_sem=recv,
            device_id={"ctx": target},
        ).start()

    def down(bz, carry):
        own(column_sem.at[z], block(bz, y, x, core))
        return carry

    def ready(bz, carry):
        pl.semaphore_signal(ready_sem.at[z], inc=1, device_id={"ctx": block(bz, y, x, core)})
        return carry

    def reach(target, carry):
        pl.semaphore_signal(reach_sem, inc=1, device_id={"ctx": target * 2 + core})
        return carry

    entered = z + x + y + core
    pl.when(entered > 0)(lambda: pl.semaphore_wait(barrier, entered))
    lax.fori_loop(0, z, down, 0)

    plane_sems = (plane_sem, plane_sem, pair_sem)
    for step, (side, target) in enumerate(peers):

        @pl.when(side == 1)
        def _(target=target, step=step):
            pl.semaphore_signal(near_sem.at[step], inc=1, device_id={"ctx": target})
            own(plane_sems[step].at[z], target)

    lax.fori_loop(0, z, ready, 0)
    d_copy = local(2, dq_hbm, dq_ref)
    len_copy = local(3, len_hbm, len_ref)
    pt_copy = local(4, pt_hbm, pt_ref)
    c_copy = local(1, ct_hbm, ct)
    q_copy = local(5, qt_hbm, qt)
    for step, (side, target) in enumerate(peers):

        @pl.when(side == 0)
        def _(target=target, step=step):
            pl.semaphore_wait(near_sem.at[step], 1)
            own(plane_sems[step].at[z], target)
            if step == 0:
                pl.semaphore_signal(near_sem.at[0], inc=1, device_id={"ctx": target})

    own_copy.wait()
    c_copy.wait()
    d_copy.wait()
    len_copy.wait()
    pt_copy.wait()
    latent = held[chip, core]
    row_page = (me * rows + lax.broadcasted_iota(jnp.int32, (1, rows), 1)) // PAGE
    first_page = me * rows // PAGE
    request_of = jnp.zeros((1, rows), jnp.int32)
    for p in range(max(1, rows // PAGE)):
        page = first_page + p
        request = (pt_ref[0, page] * POOL + pt_ref[1, page]) % REQ
        request_of = jnp.where(row_page == page, request, request_of)
    positions = me * cache_dev + lax.broadcasted_iota(jnp.int32, (1, cache_dev), 1)
    for r in range(REQ):
        queries = dq_ref[r]
        keys = ct[r]
        scores = jnp.dot(queries, keys, preferred_element_type=jnp.float32) * SCALE
        page_scores = (
            lax.dot_general(queries, latent, NT, preferred_element_type=jnp.float32) * SCALE
        )
        ok = positions < len_ref[r]
        page_ok = request_of == r
        scores = jnp.where(ok, scores, NEG)
        page_scores = jnp.where(page_ok, page_scores, NEG)
        top = jnp.maximum(
            jnp.max(scores, axis=1, keepdims=True), jnp.max(page_scores, axis=1, keepdims=True)
        )
        weights = jnp.where(ok, jnp.exp(scores - top), 0.0)
        page_weights = jnp.where(page_ok, jnp.exp(page_scores - top), 0.0)
        total = jnp.sum(weights, axis=1, keepdims=True) + jnp.sum(
            page_weights, axis=1, keepdims=True
        )
        mixed = lax.dot_general(
            weights.astype(jnp.bfloat16), keys[:D_LAT], NT, preferred_element_type=jnp.float32
        ) + jnp.dot(
            page_weights.astype(jnp.bfloat16),
            latent[:, :D_LAT],
            preferred_element_type=jnp.float32,
        )
        lane = lax.broadcasted_iota(jnp.int32, (heads, 128), 1)
        tail = jnp.where(lane < 64, top, total)
        parts[:, :, :, r * MSG : r * MSG + D_LAT] = mixed.reshape(chips, 2, 1, D_LAT)
        parts[:, :, :, r * MSG + D_LAT : (r + 1) * MSG] = tail.reshape(chips, 2, 1, 128)

    mate_copy = pltpu.make_async_remote_copy(
        src_ref=parts.at[:, 1 - core],
        dst_ref=mate,
        send_sem=mate_sem.at[0],
        recv_sem=mate_sem.at[1],
        device_id={"ctx": pair},
    )
    mate_copy.start()

    @pl.when(x == 1)
    def _():
        pl.semaphore_wait(near_sem.at[0], 1)

    pl.semaphore_signal(near_sem.at[3], inc=1, device_id={"ctx": y_peer})

    def part_copy(target):
        return pltpu.make_async_remote_copy(
            src_ref=joined.at[target],
            dst_ref=moved.at[chip],
            send_sem=part_sem.at[0],
            recv_sem=part_sem.at[1],
            device_id={"ctx": target * 2 + core},
        )

    def send_part(target, carry):
        part_copy(target).start()
        return carry

    def join():
        mate_copy.wait_recv()
        for r in range(REQ):
            mine = parts[:, core, :, r * MSG : (r + 1) * MSG].reshape(chips, MSG)
            other = mate[:, :, r * MSG : (r + 1) * MSG].reshape(chips, MSG)
            top_mine = mine[:, D_LAT : D_LAT + 1]
            top_other = other[:, D_LAT : D_LAT + 1]
            top = jnp.maximum(top_mine, top_other)
            sum_both = mine * jnp.exp(top_mine - top) + other * jnp.exp(top_other - top)
            lane = lax.broadcasted_iota(jnp.int32, (chips, 128), 1)
            tail = jnp.where(lane < 64, top, sum_both[:, D_LAT:])
            joined[:, :, r * MSG : r * MSG + D_LAT] = sum_both[:, :D_LAT].reshape(chips, 1, D_LAT)
            joined[:, :, r * MSG + D_LAT : (r + 1) * MSG] = tail.reshape(chips, 1, 128)
        moved[chip] = joined[chip]

    quarter = span // 4
    group = n // 4

    def score(i, side=None):
        pairs, before = (i + 1) * group // 2, i * group // 2 * rows
        if side is None:
            keys = held[:pairs].reshape(pairs * 2 * rows, held.shape[3])
            before = before * 2
        else:
            keys = held[:pairs, side].reshape(pairs * rows, held.shape[3])
        scores = lax.dot_general(
            q[i * quarter : (i + 1) * quarter], keys, NT, preferred_element_type=jnp.float32
        )
        fresh = keys.shape[0] - before
        col = lax.broadcasted_iota(jnp.int32, (1, fresh), 1)
        if side is not None:
            col = col + (col // rows + side) * rows
        row = lax.broadcasted_iota(jnp.int32, (quarter, fresh), 0)
        last = jnp.where(col <= row, scores[:, before:], NEG)
        if i:
            last = jnp.concatenate([scores[:, :before], last], axis=1)
        return i, keys, last

    def wide(value, count):
        return jnp.concatenate([value] * (count // 128), axis=1)

    def weigh(i, keys, scores, first, last):
        here = slice(i * quarter, (i + 1) * quarter)
        top = jnp.broadcast_to(jnp.max(scores, axis=1, keepdims=True), (quarter, 128))
        if not first:
            old = tops[here, :]
            top = jnp.maximum(top, old)
            fade = jnp.exp((old - top) * SCALE)
        weights = jnp.exp((scores - wide(top, scores.shape[1])) * SCALE)
        total = jnp.broadcast_to(jnp.sum(weights, axis=1, keepdims=True), (quarter, 128))
        mixed = jnp.dot(
            weights.astype(jnp.bfloat16), keys[:, :D_LAT], preferred_element_type=jnp.float32
        )
        if not first:
            total = total + sums[here, :] * fade
            mixed = mixed + acc[here, :] * wide(fade, D_LAT)
        if last:
            pout_ref[here, :] = (mixed * wide(1.0 / total, D_LAT)).astype(jnp.bfloat16)
        else:
            tops[here, :] = top
            sums[here, :] = total
            acc[here, :] = mixed

    def attend(side, first, last):
        scored = score(0, side)
        for i in range(1, 4):
            after = score(i, side)
            weigh(*scored, first, last)
            scored = after
        weigh(*scored, first, last)

    parts_all = moved.at[pl.ds(0, chips - 1)]

    def decode_finish():
        pltpu.make_async_copy(parts_all, parts_all, part_sem.at[1]).wait()
        for r in range(REQ):
            piece = moved[:, :, r * MSG : (r + 1) * MSG].reshape(chips, MSG)
            best = piece[:, D_LAT : D_LAT + 1]
            mass = piece[:, D_LAT + 64 : D_LAT + 65]
            factor = jnp.exp(best - jnp.max(best, axis=0, keepdims=True))
            own_sum = jnp.sum(mass * factor, axis=0, keepdims=True)
            own_out = jnp.sum(piece[:, :D_LAT] * factor, axis=0, keepdims=True)
            dout_ref[r : r + 1, :] = (own_out / own_sum).astype(jnp.bfloat16)

    def send_parts():
        pl.when(z < line - 1)(lambda: pl.semaphore_wait(reach_sem, 4 * (line - 1 - z)))
        lax.fori_loop(4 * z, chip, send_part, 0)
        lax.fori_loop(chip + 1, chips, send_part, 0)

    def await_group(p):
        for bz in range(p * (line // 4), (p + 1) * (line // 4)):
            blocks_wait(pair_sem.at[bz], 4)

    def up_all(first):
        for step in range(first, line):
            up_step(step)

    def transpose_queries():
        q_copy.wait()
        for start in range(0, span, 128):
            q[start : start + 128, :] = qt[:, start : start + 128].T

    pl.when(z > 0)(lambda: up_all(1))
    transpose_queries()
    @pl.when(z == 0)
    def _():
        up_step(1)
        column_step(1, False)
        plane_step(0)
        up_step(2)

    join()

    @pl.when(z > 0)
    def _():
        pl.semaphore_wait(near_sem.at[3], 1)
        lax.fori_loop(0, 4 * z, send_part, 0)
        lax.fori_loop(0, 4 * z, reach, 0)

    pl.when(z == 0)(lambda: pl.semaphore_wait(near_sem.at[3], 1))
    pl.when(z == 0)(lambda: up_all(3))
    for step in range(1, line):
        if step == 1:
            pl.when((z > 0) & (z + 1 < line))(lambda: column_step(z + 1, False))
            pl.when(z > 0)(lambda: column_step(z - 1, False))
            pl.when(z > 0)(lambda: plane_step(z))
        else:
            both(step, lambda bz: column_step(bz, True))
    both(1, lambda bz: plane_step(bz, False))
    pl.when(core == 0)(send_parts)
    diag_step(z)
    for step in range(2, line - 1):
        both(step, lambda bz: plane_step(bz, True))
    pl.when(z == 0)(lambda: plane_step(line - 1, True))
    pl.when(z == line - 1)(lambda: plane_step(0, True))
    for step in range(1, line):
        both(step, diag_step)

    pl.when(core == 1)(send_parts)
    pl.when(core == 1)(lambda: attend(1, True, False))
    pl.when(core == 1)(decode_finish)
    for p in range(4):
        await_group(p)
    pl.when(core == 0)(lambda: attend(None, True, True))
    pl.when(core == 1)(lambda: attend(0, False, True))

    pl.when(core == 0)(decode_finish)
    blocks_wait(send_sem, n - 2)
    blocks_wait(send_sem, 1)
    mate_copy.wait_send()
    pltpu.make_async_copy(parts_all, parts_all, part_sem.at[0]).wait()


def store(prefill_ref, decode_ref, prefill_hbm, decode_hbm, sem):
    copies = (
        pltpu.make_async_copy(decode_ref, decode_hbm, sem.at[0]),
        pltpu.make_async_copy(prefill_ref, prefill_hbm, sem.at[1]),
    )
    for copy in copies:
        copy.start()
    for copy in copies:
        copy.wait()


def shards(n, prefill_query, prefill_latent, decode_query, cache, lengths, page_table):
    span, head_here, width = prefill_query.shape
    rows = prefill_latent.shape[0]
    heads = decode_query.shape[1]
    cache_dev = cache.shape[1]
    if head_here != 1 or n % 32 or rows * n != span or span % 512:
        raise ValueError("unexpected sizes")
    line = n // 8
    vmem = pl.BlockSpec(memory_space=pltpu.VMEM)
    anywhere = pl.BlockSpec(memory_space=pl.ANY)
    dma = pltpu.SemaphoreType.DMA
    prefill_out, decode_out = pl.pallas_call(
        functools.partial(kernel, n),
        out_shape=(
            pltpu.VMEM((span, D_LAT), jnp.bfloat16),
            pltpu.VMEM((REQ, D_LAT), jnp.bfloat16),
        ),
        in_specs=[anywhere] * 6,
        out_specs=(vmem, vmem),
        scratch_shapes=[
            pltpu.VMEM((n // 2, 2, rows, width), jnp.bfloat16),
            pltpu.VMEM((REQ, heads, width), jnp.bfloat16),
            pltpu.VMEM((width, span), jnp.bfloat16),
            pltpu.VMEM((span, width), jnp.bfloat16),
            pltpu.VMEM((REQ, width, cache_dev), jnp.bfloat16),
            pltpu.SMEM(lengths.shape, jnp.int32),
            pltpu.SMEM(page_table.shape[::-1], jnp.int32),
            pltpu.VMEM((n // 2, 2, 1, REQ * MSG), jnp.float32),
            pltpu.VMEM((n // 2, 1, REQ * MSG), jnp.float32),
            pltpu.VMEM((n // 2, 1, REQ * MSG), jnp.float32),
            pltpu.VMEM((n // 2, 1, REQ * MSG), jnp.float32),
            pltpu.VMEM((span, D_LAT), jnp.float32),
            pltpu.VMEM((span, 128), jnp.float32),
            pltpu.VMEM((span, 128), jnp.float32),
            dma((6,)),
            dma,
            dma((line,)),
            dma((line,)),
            dma((line,)),
            dma((line,)),
            dma((2,)),
            dma((2,)),
            pltpu.SemaphoreType.REGULAR((line,)),
            pltpu.SemaphoreType.REGULAR((4,)),
            pltpu.SemaphoreType.REGULAR,
        ],
        compiler_params=pltpu.CompilerParams(collective_id=0, has_side_effects=True),
    )(
        prefill_query[:, 0, :].T,
        prefill_latent,
        decode_query,
        jnp.swapaxes(cache, 1, 2),
        lengths,
        page_table.T,
    )
    prefill_out, decode_out = pl.pallas_call(
        store,
        out_shape=(
            jax.ShapeDtypeStruct((span, D_LAT), jnp.bfloat16),
            jax.ShapeDtypeStruct((REQ, D_LAT), jnp.bfloat16),
        ),
        in_specs=[vmem, vmem],
        out_specs=(anywhere, anywhere),
        scratch_shapes=[dma((2,))],
    )(*(pltpu.with_memory_space_constraint(a, pltpu.VMEM) for a in (prefill_out, decode_out)))
    return prefill_out[:, None, :], decode_out[:, None, :]


def solution(mesh):
    in_specs = (
        P("groups", "ctx", None),
        P(("groups", "ctx"), None),
        P("groups", None, None),
        P("groups", "ctx", None),
        P("groups"),
        P("groups", None),
    )
    out_specs = (P("groups", "ctx", None), P("groups", "ctx", None))
    return jax.shard_map(
        functools.partial(shards, mesh.shape["ctx"]),
        mesh=mesh,
        in_specs=in_specs,
        out_specs=out_specs,
        check_vma=False,
    )
```

```python
import functools

import jax
import jax.numpy as jnp
from jax import lax
from jax.experimental import pallas as pl
from jax.experimental.pallas import tpu as pltpu
from jax.sharding import PartitionSpec as P

D_LAT = 512
PAGE = 16
POOL = 16
REQ = 2

SCALE = 192.0 ** (-0.5)
NEG = -1e30
VMEM_LIMIT = 56 * 2**20
MSG = D_LAT + 128
NT = (((1,), (1,)), ((), ()))


def score(refs, i, side):
    held, q, acc, tops, sums = refs
    rows = held.shape[2]
    quarter, group = q.shape[0] // 4, held.shape[0] // 2
    pairs, before = (i + 1) * group // 2, i * group // 2 * rows
    if side is None:
        keys = held[:pairs].reshape(pairs * 2 * rows, held.shape[3])
        before = before * 2
    else:
        keys = held[:pairs, side].reshape(pairs * rows, held.shape[3])
    scores = lax.dot_general(
        q[i * quarter : (i + 1) * quarter], keys, NT, preferred_element_type=jnp.float32
    )
    fresh = keys.shape[0] - before
    col = lax.broadcasted_iota(jnp.int32, (1, fresh), 1)
    if side is not None:
        col = col + (col // rows + side) * rows
    row = lax.broadcasted_iota(jnp.int32, (quarter, fresh), 0)
    last = jnp.where(col <= row, scores[:, before:], NEG)
    if i:
        last = jnp.concatenate([scores[:, :before], last], axis=1)
    return i, keys, last


def wide(value, count):
    return jnp.concatenate([value] * (count // 128), axis=1)


def weigh(refs, i, keys, scores, first, emit):
    held, q, acc, tops, sums = refs
    quarter = q.shape[0] // 4
    here = slice(i * quarter, (i + 1) * quarter)
    top = jnp.broadcast_to(jnp.max(scores, axis=1, keepdims=True), (quarter, 128))
    if not first:
        old = tops[here, :]
        top = jnp.maximum(top, old)
        fade = jnp.exp((old - top) * SCALE)
    weights = jnp.exp((scores - wide(top, scores.shape[1])) * SCALE)
    total = jnp.broadcast_to(jnp.sum(weights, axis=1, keepdims=True), (quarter, 128))
    mixed = jnp.dot(
        weights.astype(jnp.bfloat16), keys[:, :D_LAT], preferred_element_type=jnp.float32
    )
    if not first:
        total = total + sums[here, :] * fade
        mixed = mixed + acc[here, :] * wide(fade, D_LAT)
    if emit is not None:
        emit(i, (mixed * wide(1.0 / total, D_LAT)).astype(jnp.bfloat16))
    else:
        tops[here, :] = top
        sums[here, :] = total
        acc[here, :] = mixed


def attend(refs, side, first, emit):
    scored = score(refs, 0, side)
    for i in range(1, 4):
        after = score(refs, i, side)
        weigh(refs, *scored, first, emit)
        scored = after
    weigh(refs, *scored, first, emit)


def kernel(
    n,
    qt_hbm,
    lat_hbm,
    dq_hbm,
    ct_hbm,
    len_hbm,
    pt_hbm,
    held,
    q,
    acc,
    tops,
    sums,
    pout_ref,
    dout_ref,
    dq_ref,
    qt,
    ct,
    len_ref,
    pt_ref,
    parts,
    mate,
    joined,
    moved,
    local_sem,
    send_sem,
    column_sem,
    plane_sem,
    diag_sem,
    pair_sem,
    part_sem,
    mate_sem,
    ready_sem,
    near_sem,
    reach_sem,
):
    me = lax.axis_index("ctx")
    line = n // 8
    core = me % 2
    x = (me // 2) % 2
    y = (me // 4) % 2
    z = me // 8
    far_x, far_y = 1 - x, 1 - y
    rows = lat_hbm.shape[0]
    heads = dq_ref.shape[1]
    chips = n // 2
    chip = me // 2
    span = qt.shape[1]
    cache_dev = ct.shape[2]
    split = rows // 2 if rows % 32 == 0 else rows

    def block(bz, by, bx, bc):
        return ((bz * 2 + by) * 2 + bx) * 2 + bc

    x_peer = block(z, y, far_x, core)
    y_peer = block(z, far_y, x, core)
    pair = block(z, y, x, 1 - core)

    def local(index, source, target):
        copy = pltpu.make_async_copy(source, target, local_sem.at[index])
        copy.start()
        return copy

    own_copy = local(0, lat_hbm, held.at[chip, core])

    barrier = pltpu.get_barrier_semaphore()
    peers = ((x, x_peer), (y, y_peer), (core, pair))
    for side, target in peers:

        @pl.when(side == 0)
        def _(target=target):
            pl.semaphore_signal(barrier, inc=1, device_id={"ctx": target})

    def greet(bz, carry):
        pl.semaphore_signal(barrier, inc=1, device_id={"ctx": block(bz, y, x, core)})
        return carry

    lax.fori_loop(z + 1, line, greet, 0)


    def both(distance, act):
        if distance == 0:
            act(z)
            return
        pl.when(z >= distance)(lambda: act(z - distance))
        pl.when(z + distance < line)(lambda: act(z + distance))

    def move(index, recv, target, part=None):
        ref = held.at[index // 2, index % 2]
        if part == 0:
            ref = held.at[index // 2, index % 2, pl.ds(0, split)]
        if part == 1:
            ref = held.at[index // 2, index % 2, pl.ds(split, rows - split)]
        pltpu.make_async_remote_copy(
            src_ref=ref, dst_ref=ref, send_sem=send_sem, recv_sem=recv, device_id={"ctx": target}
        ).start()

    def blocks_wait(sem, count):
        ref = held.at[0, 0] if count == 1 else held.at[pl.ds(0, count // 2)]
        pltpu.make_async_copy(ref, ref, sem).wait()

    def to_pair(bz, by, bx):
        index = block(bz, by, bx, core)
        move(index, pair_sem.at[bz], pair)

    def spread(bz, straight):
        index = block(bz, y, x, core)
        move(index, plane_sem.at[bz], x_peer)
        move(index, plane_sem.at[bz], y_peer)
        if straight:
            move(index, diag_sem.at[bz], block(z, far_y, far_x, core))
        to_pair(bz, y, x)

    def column_step(bz, straight):
        blocks_wait(column_sem.at[bz], 1)
        spread(bz, straight)

    def relay_y(bz):
        if split < rows:
            move(block(bz, y, far_x, core), diag_sem.at[bz], y_peer, 1)

    def relay_x(bz):
        move(block(bz, far_y, x, core), diag_sem.at[bz], x_peer, 0)

    def plane_step(bz, straight=False):
        blocks_wait(plane_sem.at[bz], 2)
        if not straight:
            relay_y(bz)
            relay_x(bz)
        to_pair(bz, y, far_x)
        to_pair(bz, far_y, x)

    def diag_step(bz):
        blocks_wait(diag_sem.at[bz], 1)
        to_pair(bz, far_y, far_x)

    def up_step(distance):
        @pl.when(z + distance < line)
        def _():
            pl.semaphore_wait(ready_sem.at[z + distance], 1)
            own(column_sem.at[z], block(z + distance, y, x, core))

    def own(recv, target):
        pltpu.make_async_remote_copy(
            src_ref=lat_hbm,
            dst_ref=held.at[chip, core],
            send_sem=send_sem,
            recv_sem=recv,
            device_id={"ctx": target},
        ).start()

    def down(bz, carry):
        own(column_sem.at[z], block(bz, y, x, core))
        return carry

    def ready(bz, carry):
        pl.semaphore_signal(ready_sem.at[z], inc=1, device_id={"ctx": block(bz, y, x, core)})
        return carry

    def reach(target, carry):
        pl.semaphore_signal(reach_sem, inc=1, device_id={"ctx": target * 2 + core})
        return carry

    entered = z + x + y + core
    pl.when(entered > 0)(lambda: pl.semaphore_wait(barrier, entered))
    lax.fori_loop(0, z, down, 0)

    plane_sems = (plane_sem, plane_sem, pair_sem)
    for step, (side, target) in enumerate(peers):

        @pl.when(side == 1)
        def _(target=target, step=step):
            pl.semaphore_signal(near_sem.at[step], inc=1, device_id={"ctx": target})
            own(plane_sems[step].at[z], target)

    lax.fori_loop(0, z, ready, 0)
    d_copy = local(2, dq_hbm, dq_ref)
    len_copy = local(3, len_hbm, len_ref)
    pt_copy = local(4, pt_hbm, pt_ref)
    c_copy = local(1, ct_hbm, ct)
    q_copy = local(5, qt_hbm, qt)
    for step, (side, target) in enumerate(peers):

        @pl.when(side == 0)
        def _(target=target, step=step):
            pl.semaphore_wait(near_sem.at[step], 1)
            own(plane_sems[step].at[z], target)
            if step == 0:
                pl.semaphore_signal(near_sem.at[0], inc=1, device_id={"ctx": target})

    own_copy.wait()
    c_copy.wait()
    d_copy.wait()
    len_copy.wait()
    pt_copy.wait()
    latent = held[chip, core]
    row_page = (me * rows + lax.broadcasted_iota(jnp.int32, (1, rows), 1)) // PAGE
    first_page = me * rows // PAGE
    request_of = jnp.zeros((1, rows), jnp.int32)
    for p in range(max(1, rows // PAGE)):
        page = first_page + p
        request = (pt_ref[0, page] * POOL + pt_ref[1, page]) % REQ
        request_of = jnp.where(row_page == page, request, request_of)
    positions = me * cache_dev + lax.broadcasted_iota(jnp.int32, (1, cache_dev), 1)
    for r in range(REQ):
        queries = dq_ref[r]
        keys = ct[r]
        scores = jnp.dot(queries, keys, preferred_element_type=jnp.float32) * SCALE
        page_scores = (
            lax.dot_general(queries, latent, NT, preferred_element_type=jnp.float32) * SCALE
        )
        ok = positions < len_ref[r]
        page_ok = request_of == r
        scores = jnp.where(ok, scores, NEG)
        page_scores = jnp.where(page_ok, page_scores, NEG)
        top = jnp.maximum(
            jnp.max(scores, axis=1, keepdims=True), jnp.max(page_scores, axis=1, keepdims=True)
        )
        weights = jnp.where(ok, jnp.exp(scores - top), 0.0)
        page_weights = jnp.where(page_ok, jnp.exp(page_scores - top), 0.0)
        total = jnp.sum(weights, axis=1, keepdims=True) + jnp.sum(
            page_weights, axis=1, keepdims=True
        )
        mixed = lax.dot_general(
            weights.astype(jnp.bfloat16), keys[:D_LAT], NT, preferred_element_type=jnp.float32
        ) + jnp.dot(
            page_weights.astype(jnp.bfloat16),
            latent[:, :D_LAT],
            preferred_element_type=jnp.float32,
        )
        lane = lax.broadcasted_iota(jnp.int32, (heads, 128), 1)
        tail = jnp.where(lane < 64, top, total)
        parts[:, :, :, r * MSG : r * MSG + D_LAT] = mixed.reshape(chips, 2, 1, D_LAT)
        parts[:, :, :, r * MSG + D_LAT : (r + 1) * MSG] = tail.reshape(chips, 2, 1, 128)

    mate_copy = pltpu.make_async_remote_copy(
        src_ref=parts.at[:, 1 - core],
        dst_ref=mate,
        send_sem=mate_sem.at[0],
        recv_sem=mate_sem.at[1],
        device_id={"ctx": pair},
    )
    mate_copy.start()

    @pl.when(x == 1)
    def _():
        pl.semaphore_wait(near_sem.at[0], 1)

    pl.semaphore_signal(near_sem.at[3], inc=1, device_id={"ctx": y_peer})

    def part_copy(target):
        return pltpu.make_async_remote_copy(
            src_ref=joined.at[target],
            dst_ref=moved.at[chip],
            send_sem=part_sem.at[0],
            recv_sem=part_sem.at[1],
            device_id={"ctx": target * 2 + core},
        )

    def send_part(target, carry):
        part_copy(target).start()
        return carry

    def join():
        mate_copy.wait_recv()
        for r in range(REQ):
            mine = parts[:, core, :, r * MSG : (r + 1) * MSG].reshape(chips, MSG)
            other = mate[:, :, r * MSG : (r + 1) * MSG].reshape(chips, MSG)
            top_mine = mine[:, D_LAT : D_LAT + 1]
            top_other = other[:, D_LAT : D_LAT + 1]
            top = jnp.maximum(top_mine, top_other)
            sum_both = mine * jnp.exp(top_mine - top) + other * jnp.exp(top_other - top)
            lane = lax.broadcasted_iota(jnp.int32, (chips, 128), 1)
            tail = jnp.where(lane < 64, top, sum_both[:, D_LAT:])
            joined[:, :, r * MSG : r * MSG + D_LAT] = sum_both[:, :D_LAT].reshape(chips, 1, D_LAT)
            joined[:, :, r * MSG + D_LAT : (r + 1) * MSG] = tail.reshape(chips, 1, 128)
        moved[chip] = joined[chip]

    quarter = span // 4
    group = n // 4

    parts_all = moved.at[pl.ds(0, chips - 1)]

    def decode_finish():
        pltpu.make_async_copy(parts_all, parts_all, part_sem.at[1]).wait()
        for r in range(REQ):
            piece = moved[:, :, r * MSG : (r + 1) * MSG].reshape(chips, MSG)
            best = piece[:, D_LAT : D_LAT + 1]
            mass = piece[:, D_LAT + 64 : D_LAT + 65]
            factor = jnp.exp(best - jnp.max(best, axis=0, keepdims=True))
            own_sum = jnp.sum(mass * factor, axis=0, keepdims=True)
            own_out = jnp.sum(piece[:, :D_LAT] * factor, axis=0, keepdims=True)
            dout_ref[r : r + 1, :] = (own_out / own_sum).astype(jnp.bfloat16)

    def send_parts():
        pl.when(z < line - 1)(lambda: pl.semaphore_wait(reach_sem, 4 * (line - 1 - z)))
        lax.fori_loop(4 * z, chip, send_part, 0)
        lax.fori_loop(chip + 1, chips, send_part, 0)

    def await_group(p):
        for bz in range(p * (line // 4), (p + 1) * (line // 4)):
            blocks_wait(pair_sem.at[bz], 4)

    def up_all(first):
        for step in range(first, line):
            up_step(step)

    def transpose_queries():
        q_copy.wait()
        for start in range(0, span, 128):
            q[start : start + 128, :] = qt[:, start : start + 128].T

    pl.when(z > 0)(lambda: up_all(1))
    transpose_queries()
    @pl.when(z == 0)
    def _():
        up_step(1)
        column_step(1, False)
        plane_step(0)
        up_step(2)

    join()

    @pl.when(z > 0)
    def _():
        pl.semaphore_wait(near_sem.at[3], 1)
        lax.fori_loop(0, 4 * z, send_part, 0)
        lax.fori_loop(0, 4 * z, reach, 0)

    pl.when(z == 0)(lambda: pl.semaphore_wait(near_sem.at[3], 1))
    pl.when(z == 0)(lambda: up_all(3))
    for step in range(1, line):
        if step == 1:
            pl.when(z > 0)(lambda: column_step(z - 1, False))
            pl.when((z > 0) & (z + 1 < line))(lambda: column_step(z + 1, False))
            pl.when(z > 0)(lambda: plane_step(z))
        else:
            both(step, lambda bz: column_step(bz, True))
    both(1, lambda bz: plane_step(bz, False))
    pl.when(core == 0)(send_parts)
    diag_step(z)
    for step in range(2, line - 1):
        both(step, lambda bz: plane_step(bz, True))
    pl.when(z == 0)(lambda: plane_step(line - 1, True))
    pl.when(z == line - 1)(lambda: plane_step(0, True))
    for step in range(1, line):
        both(step, diag_step)

    pl.when(core == 1)(send_parts)
    refs = (held, q, acc, tops, sums)
    pl.when(core == 1)(lambda: attend(refs, 1, True, None))
    pl.when(core == 1)(decode_finish)
    for p in range(4):
        await_group(p)


    def emit(i, value):
        pout_ref[i * quarter : (i + 1) * quarter, :] = value

    pl.when(core == 0)(lambda: attend(refs, None, True, emit))
    pl.when(core == 0)(decode_finish)
    blocks_wait(send_sem, n - 2)
    blocks_wait(send_sem, 1)
    mate_copy.wait_send()
    pltpu.make_async_copy(parts_all, parts_all, part_sem.at[0]).wait()


def store(
    held, q, acc, tops, sums, whole_ref, decode_ref, prefill_hbm, decode_hbm, rows_ref, sem
):
    quarter = q.shape[0] // 4
    core = lax.axis_index("ctx") % 2
    decode_copy = pltpu.make_async_copy(decode_ref, decode_hbm, sem.at[4])
    decode_copy.start()

    def chunk_copy(i):
        here = pl.ds(i * quarter, quarter)
        return pltpu.make_async_copy(rows_ref.at[here], prefill_hbm.at[here], sem.at[i])

    def emit(i, value):
        rows_ref[i * quarter : (i + 1) * quarter, :] = value
        chunk_copy(i).start()

    @pl.when(core == 0)
    def _():
        copy = pltpu.make_async_copy(whole_ref, prefill_hbm, sem.at[0])
        copy.start()
        copy.wait()

    @pl.when(core == 1)
    def _():
        attend((held, q, acc, tops, sums), 0, False, emit)
        for i in range(4):
            chunk_copy(i).wait()

    decode_copy.wait()


def shards(n, prefill_query, prefill_latent, decode_query, cache, lengths, page_table):
    span, head_here, width = prefill_query.shape
    rows = prefill_latent.shape[0]
    heads = decode_query.shape[1]
    cache_dev = cache.shape[1]
    if head_here != 1 or n % 32 or rows * n != span or span % 512:
        raise ValueError("unexpected sizes")
    line = n // 8
    vmem = pl.BlockSpec(memory_space=pltpu.VMEM)
    anywhere = pl.BlockSpec(memory_space=pl.ANY)
    dma = pltpu.SemaphoreType.DMA
    state = pl.pallas_call(
        functools.partial(kernel, n),
        out_shape=(
            pltpu.VMEM((n // 2, 2, rows, width), jnp.bfloat16),
            pltpu.VMEM((span, width), jnp.bfloat16),
            pltpu.VMEM((span, D_LAT), jnp.float32),
            pltpu.VMEM((span, 128), jnp.float32),
            pltpu.VMEM((span, 128), jnp.float32),
            pltpu.VMEM((span, D_LAT), jnp.bfloat16),
            pltpu.VMEM((REQ, D_LAT), jnp.bfloat16),
        ),
        in_specs=[anywhere] * 6,
        out_specs=(vmem,) * 7,
        scratch_shapes=[
            pltpu.VMEM((REQ, heads, width), jnp.bfloat16),
            pltpu.VMEM((width, span), jnp.bfloat16),
            pltpu.VMEM((REQ, width, cache_dev), jnp.bfloat16),
            pltpu.SMEM(lengths.shape, jnp.int32),
            pltpu.SMEM(page_table.shape[::-1], jnp.int32),
            pltpu.VMEM((n // 2, 2, 1, REQ * MSG), jnp.float32),
            pltpu.VMEM((n // 2, 1, REQ * MSG), jnp.float32),
            pltpu.VMEM((n // 2, 1, REQ * MSG), jnp.float32),
            pltpu.VMEM((n // 2, 1, REQ * MSG), jnp.float32),
            dma((6,)),
            dma,
            dma((line,)),
            dma((line,)),
            dma((line,)),
            dma((line,)),
            dma((2,)),
            dma((2,)),
            pltpu.SemaphoreType.REGULAR((line,)),
            pltpu.SemaphoreType.REGULAR((4,)),
            pltpu.SemaphoreType.REGULAR,
        ],
        compiler_params=pltpu.CompilerParams(
            collective_id=0, has_side_effects=True, vmem_limit_bytes=VMEM_LIMIT
        ),
    )(
        prefill_query[:, 0, :].T,
        prefill_latent,
        decode_query,
        jnp.swapaxes(cache, 1, 2),
        lengths,
        page_table.T,
    )
    prefill_out, decode_out = pl.pallas_call(
        store,
        out_shape=(
            jax.ShapeDtypeStruct((span, D_LAT), jnp.bfloat16),
            jax.ShapeDtypeStruct((REQ, D_LAT), jnp.bfloat16),
        ),
        in_specs=[vmem] * 7,
        out_specs=(anywhere, anywhere),
        scratch_shapes=[pltpu.VMEM((span, D_LAT), jnp.bfloat16), dma((5,))],
        compiler_params=pltpu.CompilerParams(vmem_limit_bytes=VMEM_LIMIT),
    )(*(pltpu.with_memory_space_constraint(a, pltpu.VMEM) for a in state))
    return prefill_out[:, None, :], decode_out[:, None, :]


def solution(mesh):
    in_specs = (
        P("groups", "ctx", None),
        P(("groups", "ctx"), None),
        P("groups", None, None),
        P("groups", "ctx", None),
        P("groups"),
        P("groups", None),
    )
    out_specs = (P("groups", "ctx", None), P("groups", "ctx", None))
    return jax.shard_map(
        functools.partial(shards, mesh.shape["ctx"]),
        mesh=mesh,
        in_specs=in_specs,
        out_specs=out_specs,
        check_vma=False,
    )
```

```python
import functools

import jax
import jax.numpy as jnp
from jax import lax
from jax.experimental import pallas as pl
from jax.experimental.pallas import tpu as pltpu
from jax.sharding import PartitionSpec as P

D_LAT = 512
PAGE = 16
POOL = 16
REQ = 2

SCALE = 192.0 ** (-0.5)
NEG = -1e30
VMEM_LIMIT = 56 * 2**20
MSG = D_LAT + 128
NT = (((1,), (1,)), ((), ()))


def score(refs, i, side):
    held, q, acc, tops, sums = refs
    rows = held.shape[2]
    quarter, group = q.shape[0] // 4, held.shape[0] // 2
    pairs, before = (i + 1) * group // 2, i * group // 2 * rows
    if side is None:
        keys = held[:pairs].reshape(pairs * 2 * rows, held.shape[3])
        before = before * 2
    else:
        keys = held[:pairs, side].reshape(pairs * rows, held.shape[3])
    scores = lax.dot_general(
        q[i * quarter : (i + 1) * quarter], keys, NT, preferred_element_type=jnp.float32
    )
    fresh = keys.shape[0] - before
    col = lax.broadcasted_iota(jnp.int32, (1, fresh), 1)
    if side is not None:
        col = col + (col // rows + side) * rows
    row = lax.broadcasted_iota(jnp.int32, (quarter, fresh), 0)
    last = jnp.where(col <= row, scores[:, before:], NEG)
    if i:
        last = jnp.concatenate([scores[:, :before], last], axis=1)
    return i, keys, last


def wide(value, count):
    return jnp.concatenate([value] * (count // 128), axis=1)


def weigh(refs, i, keys, scores, first, emit):
    held, q, acc, tops, sums = refs
    quarter = q.shape[0] // 4
    here = slice(i * quarter, (i + 1) * quarter)
    top = jnp.broadcast_to(jnp.max(scores, axis=1, keepdims=True), (quarter, 128))
    if not first:
        old = tops[here, :]
        top = jnp.maximum(top, old)
        fade = jnp.exp((old - top) * SCALE)
    weights = jnp.exp((scores - wide(top, scores.shape[1])) * SCALE)
    total = jnp.broadcast_to(jnp.sum(weights, axis=1, keepdims=True), (quarter, 128))
    mixed = jnp.dot(
        weights.astype(jnp.bfloat16), keys[:, :D_LAT], preferred_element_type=jnp.float32
    )
    if not first:
        total = total + sums[here, :] * fade
        mixed = mixed + acc[here, :] * wide(fade, D_LAT)
    if emit is not None:
        emit(i, (mixed * wide(1.0 / total, D_LAT)).astype(jnp.bfloat16))
    else:
        tops[here, :] = top
        sums[here, :] = total
        acc[here, :] = mixed


def attend(refs, side, first, emit):
    scored = score(refs, 3, side)
    for i in (2, 1, 0):
        after = score(refs, i, side)
        weigh(refs, *scored, first, emit)
        scored = after
    weigh(refs, *scored, first, emit)


def kernel(
    n,
    qt_hbm,
    lat_hbm,
    dq_hbm,
    ct_hbm,
    len_hbm,
    pt_hbm,
    held,
    q,
    acc,
    tops,
    sums,
    pout_ref,
    dout_ref,
    dq_ref,
    qt,
    ct,
    len_ref,
    pt_ref,
    parts,
    mate,
    joined,
    moved,
    local_sem,
    send_sem,
    column_sem,
    plane_sem,
    diag_sem,
    pair_sem,
    part_sem,
    mate_sem,
    ready_sem,
    near_sem,
    reach_sem,
):
    me = lax.axis_index("ctx")
    line = n // 8
    core = me % 2
    x = (me // 2) % 2
    y = (me // 4) % 2
    z = me // 8
    far_x, far_y = 1 - x, 1 - y
    rows = lat_hbm.shape[0]
    heads = dq_ref.shape[1]
    chips = n // 2
    chip = me // 2
    span = qt.shape[1]
    cache_dev = ct.shape[2]
    split = rows // 2 if rows % 32 == 0 else rows

    def block(bz, by, bx, bc):
        return ((bz * 2 + by) * 2 + bx) * 2 + bc

    x_peer = block(z, y, far_x, core)
    y_peer = block(z, far_y, x, core)
    pair = block(z, y, x, 1 - core)

    def local(index, source, target):
        copy = pltpu.make_async_copy(source, target, local_sem.at[index])
        copy.start()
        return copy

    own_copy = local(0, lat_hbm, held.at[chip, core])

    barrier = pltpu.get_barrier_semaphore()
    peers = ((x, x_peer), (y, y_peer), (core, pair))
    for side, target in peers:

        @pl.when(side == 0)
        def _(target=target):
            pl.semaphore_signal(barrier, inc=1, device_id={"ctx": target})

    def greet(bz, carry):
        pl.semaphore_signal(barrier, inc=1, device_id={"ctx": block(bz, y, x, core)})
        return carry

    lax.fori_loop(z + 1, line, greet, 0)


    def both(distance, act):
        if distance == 0:
            act(z)
            return
        pl.when(z >= distance)(lambda: act(z - distance))
        pl.when(z + distance < line)(lambda: act(z + distance))

    def move(index, recv, target, part=None):
        ref = held.at[index // 2, index % 2]
        if part == 0:
            ref = held.at[index // 2, index % 2, pl.ds(0, split)]
        if part == 1:
            ref = held.at[index // 2, index % 2, pl.ds(split, rows - split)]
        pltpu.make_async_remote_copy(
            src_ref=ref, dst_ref=ref, send_sem=send_sem, recv_sem=recv, device_id={"ctx": target}
        ).start()

    def blocks_wait(sem, count):
        ref = held.at[0, 0] if count == 1 else held.at[pl.ds(0, count // 2)]
        pltpu.make_async_copy(ref, ref, sem).wait()

    def to_pair(bz, by, bx):
        index = block(bz, by, bx, core)
        move(index, pair_sem.at[bz], pair)

    def choose(condition, act):
        if condition is True:
            act()
        elif condition is not False:
            pl.when(condition)(act)

    def spread(bz, straight):
        index = block(bz, y, x, core)
        move(index, plane_sem.at[bz], x_peer)
        move(index, plane_sem.at[bz], y_peer)
        choose(straight, lambda: move(index, diag_sem.at[bz], block(z, far_y, far_x, core)))
        to_pair(bz, y, x)

    def column_step(bz, straight):
        blocks_wait(column_sem.at[bz], 1)
        spread(bz, straight)

    def relay_y(bz):
        if split < rows:
            move(block(bz, y, far_x, core), diag_sem.at[bz], y_peer, 1)

    def relay_x(bz):
        move(block(bz, far_y, x, core), diag_sem.at[bz], x_peer, 0)

    def plane_step(bz, straight=False):
        blocks_wait(plane_sem.at[bz], 2)

        def relay():
            relay_y(bz)
            relay_x(bz)

        choose(not straight if isinstance(straight, bool) else core == 1, relay)
        to_pair(bz, y, far_x)
        to_pair(bz, far_y, x)

    def diag_step(bz):
        blocks_wait(diag_sem.at[bz], 1)
        to_pair(bz, far_y, far_x)

    def up_step(distance):
        @pl.when(z + distance < line)
        def _():
            pl.semaphore_wait(ready_sem.at[z + distance], 1)
            own(column_sem.at[z], block(z + distance, y, x, core))

    def own(recv, target):
        pltpu.make_async_remote_copy(
            src_ref=lat_hbm,
            dst_ref=held.at[chip, core],
            send_sem=send_sem,
            recv_sem=recv,
            device_id={"ctx": target},
        ).start()

    def down(bz, carry):
        own(column_sem.at[z], block(bz, y, x, core))
        return carry

    def ready(bz, carry):
        pl.semaphore_signal(ready_sem.at[z], inc=1, device_id={"ctx": block(bz, y, x, core)})
        return carry

    def reach(target, carry):
        pl.semaphore_signal(reach_sem, inc=1, device_id={"ctx": target * 2 + core})
        return carry

    entered = z + x + y + core
    pl.when(entered > 0)(lambda: pl.semaphore_wait(barrier, entered))
    lax.fori_loop(0, z, down, 0)

    plane_sems = (plane_sem, plane_sem, pair_sem)
    for step, (side, target) in enumerate(peers):

        @pl.when(side == 1)
        def _(target=target, step=step):
            pl.semaphore_signal(near_sem.at[step], inc=1, device_id={"ctx": target})
            own(plane_sems[step].at[z], target)

    lax.fori_loop(0, z, ready, 0)
    d_copy = local(2, dq_hbm, dq_ref)
    len_copy = local(3, len_hbm, len_ref)
    pt_copy = local(4, pt_hbm, pt_ref)
    c_copy = local(1, ct_hbm, ct)
    q_copy = local(5, qt_hbm, qt)
    for step, (side, target) in enumerate(peers):

        @pl.when(side == 0)
        def _(target=target, step=step):
            pl.semaphore_wait(near_sem.at[step], 1)
            own(plane_sems[step].at[z], target)
            if step == 0:
                pl.semaphore_signal(near_sem.at[0], inc=1, device_id={"ctx": target})

    own_copy.wait()
    c_copy.wait()
    d_copy.wait()
    len_copy.wait()
    pt_copy.wait()
    latent = held[chip, core]
    row_page = (me * rows + lax.broadcasted_iota(jnp.int32, (1, rows), 1)) // PAGE
    first_page = me * rows // PAGE
    request_of = jnp.zeros((1, rows), jnp.int32)
    for p in range(max(1, rows // PAGE)):
        page = first_page + p
        request = (pt_ref[0, page] * POOL + pt_ref[1, page]) % REQ
        request_of = jnp.where(row_page == page, request, request_of)
    positions = me * cache_dev + lax.broadcasted_iota(jnp.int32, (1, cache_dev), 1)
    for r in range(REQ):
        queries = dq_ref[r]
        keys = ct[r]
        scores = jnp.dot(queries, keys, preferred_element_type=jnp.float32) * SCALE
        page_scores = (
            lax.dot_general(queries, latent, NT, preferred_element_type=jnp.float32) * SCALE
        )
        ok = positions < len_ref[r]
        page_ok = request_of == r
        scores = jnp.where(ok, scores, NEG)
        page_scores = jnp.where(page_ok, page_scores, NEG)
        top = jnp.maximum(
            jnp.max(scores, axis=1, keepdims=True), jnp.max(page_scores, axis=1, keepdims=True)
        )
        weights = jnp.where(ok, jnp.exp(scores - top), 0.0)
        page_weights = jnp.where(page_ok, jnp.exp(page_scores - top), 0.0)
        total = jnp.sum(weights, axis=1, keepdims=True) + jnp.sum(
            page_weights, axis=1, keepdims=True
        )
        mixed = lax.dot_general(
            weights.astype(jnp.bfloat16), keys[:D_LAT], NT, preferred_element_type=jnp.float32
        ) + jnp.dot(
            page_weights.astype(jnp.bfloat16),
            latent[:, :D_LAT],
            preferred_element_type=jnp.float32,
        )
        lane = lax.broadcasted_iota(jnp.int32, (heads, 128), 1)
        tail = jnp.where(lane < 64, top, total)
        parts[:, :, :, r * MSG : r * MSG + D_LAT] = mixed.reshape(chips, 2, 1, D_LAT)
        parts[:, :, :, r * MSG + D_LAT : (r + 1) * MSG] = tail.reshape(chips, 2, 1, 128)

    mate_copy = pltpu.make_async_remote_copy(
        src_ref=parts.at[:, 1 - core],
        dst_ref=mate,
        send_sem=mate_sem.at[0],
        recv_sem=mate_sem.at[1],
        device_id={"ctx": pair},
    )
    mate_copy.start()

    @pl.when(x == 1)
    def _():
        pl.semaphore_wait(near_sem.at[0], 1)

    pl.semaphore_signal(near_sem.at[3], inc=1, device_id={"ctx": y_peer})

    def part_copy(target):
        return pltpu.make_async_remote_copy(
            src_ref=joined.at[target],
            dst_ref=moved.at[chip],
            send_sem=part_sem.at[0],
            recv_sem=part_sem.at[1],
            device_id={"ctx": target * 2 + core},
        )

    def send_part(target, carry):
        part_copy(target).start()
        return carry

    def join():
        mate_copy.wait_recv()
        for r in range(REQ):
            mine = parts[:, core, :, r * MSG : (r + 1) * MSG].reshape(chips, MSG)
            other = mate[:, :, r * MSG : (r + 1) * MSG].reshape(chips, MSG)
            top_mine = mine[:, D_LAT : D_LAT + 1]
            top_other = other[:, D_LAT : D_LAT + 1]
            top = jnp.maximum(top_mine, top_other)
            sum_both = mine * jnp.exp(top_mine - top) + other * jnp.exp(top_other - top)
            lane = lax.broadcasted_iota(jnp.int32, (chips, 128), 1)
            tail = jnp.where(lane < 64, top, sum_both[:, D_LAT:])
            joined[:, :, r * MSG : r * MSG + D_LAT] = sum_both[:, :D_LAT].reshape(chips, 1, D_LAT)
            joined[:, :, r * MSG + D_LAT : (r + 1) * MSG] = tail.reshape(chips, 1, 128)
        moved[chip] = joined[chip]

    quarter = span // 4
    group = n // 4

    parts_all = moved.at[pl.ds(0, chips - 1)]

    def decode_finish():
        pltpu.make_async_copy(parts_all, parts_all, part_sem.at[1]).wait()
        for r in range(REQ):
            piece = moved[:, :, r * MSG : (r + 1) * MSG].reshape(chips, MSG)
            best = piece[:, D_LAT : D_LAT + 1]
            mass = piece[:, D_LAT + 64 : D_LAT + 65]
            factor = jnp.exp(best - jnp.max(best, axis=0, keepdims=True))
            own_sum = jnp.sum(mass * factor, axis=0, keepdims=True)
            own_out = jnp.sum(piece[:, :D_LAT] * factor, axis=0, keepdims=True)
            dout_ref[r : r + 1, :] = (own_out / own_sum).astype(jnp.bfloat16)

    def send_parts():
        pl.when(z < line - 1)(lambda: pl.semaphore_wait(reach_sem, 4 * (line - 1 - z)))
        lax.fori_loop(4 * z, chip, send_part, 0)
        lax.fori_loop(chip + 1, chips, send_part, 0)

    def await_group(p):
        for bz in range(p * (line // 4), (p + 1) * (line // 4)):
            blocks_wait(pair_sem.at[bz], 4)

    def up_all(first):
        for step in range(first, line):
            up_step(step)

    def transpose_queries():
        q_copy.wait()
        for start in range(0, span, 128):
            q[start : start + 128, :] = qt[:, start : start + 128].T

    pl.when(z > 0)(lambda: up_all(1))
    transpose_queries()
    @pl.when(z == 0)
    def _():
        up_step(1)
        column_step(1, False)
        plane_step(0)
        up_step(2)

    join()

    @pl.when(z > 0)
    def _():
        pl.semaphore_wait(near_sem.at[3], 1)
        lax.fori_loop(0, 4 * z, send_part, 0)
        lax.fori_loop(0, 4 * z, reach, 0)

    pl.when(z == 0)(lambda: pl.semaphore_wait(near_sem.at[3], 1))
    pl.when(z == 0)(lambda: up_all(3))
    for step in range(1, line):
        if step == 1:
            pl.when(z > 0)(lambda: column_step(z - 1, False))
            pl.when((z > 0) & (z + 1 < line))(lambda: column_step(z + 1, False))
            pl.when(z > 0)(lambda: plane_step(z))
        else:
            both(step, lambda bz, far=(core == 0) if step <= 2 else True: column_step(bz, far))
    both(1, lambda bz: plane_step(bz, False))
    pl.when(core == 0)(send_parts)
    diag_step(z)
    for step in range(2, line - 1):
        both(step, lambda bz, far=(core == 0) if step <= 2 else True: plane_step(bz, far))
    pl.when(z == 0)(lambda: plane_step(line - 1, True))
    pl.when(z == line - 1)(lambda: plane_step(0, True))
    for step in range(1, line):
        both(step, diag_step)

    pl.when(core == 1)(send_parts)
    refs = (held, q, acc, tops, sums)
    pl.when(core == 1)(lambda: attend(refs, 1, True, None))
    pl.when(core == 1)(decode_finish)
    for p in range(4):
        await_group(p)


    def emit(i, value):
        pout_ref[i * quarter : (i + 1) * quarter, :] = value

    pl.when(core == 0)(lambda: attend(refs, None, True, emit))
    pl.when(core == 0)(decode_finish)
    blocks_wait(send_sem, n - 2)
    blocks_wait(send_sem, 1)
    mate_copy.wait_send()
    pltpu.make_async_copy(parts_all, parts_all, part_sem.at[0]).wait()


def store(
    held, q, acc, tops, sums, whole_ref, decode_ref, prefill_hbm, decode_hbm, rows_ref, sem
):
    quarter = q.shape[0] // 4
    core = lax.axis_index("ctx") % 2
    decode_copy = pltpu.make_async_copy(decode_ref, decode_hbm, sem.at[4])
    decode_copy.start()

    def chunk_copy(i):
        here = pl.ds(i * quarter, quarter)
        return pltpu.make_async_copy(rows_ref.at[here], prefill_hbm.at[here], sem.at[i])

    def emit(i, value):
        rows_ref[i * quarter : (i + 1) * quarter, :] = value
        chunk_copy(i).start()

    @pl.when(core == 0)
    def _():
        copy = pltpu.make_async_copy(whole_ref, prefill_hbm, sem.at[0])
        copy.start()
        copy.wait()

    @pl.when(core == 1)
    def _():
        attend((held, q, acc, tops, sums), 0, False, emit)
        for i in range(4):
            chunk_copy(i).wait()

    decode_copy.wait()


def shards(n, prefill_query, prefill_latent, decode_query, cache, lengths, page_table):
    span, head_here, width = prefill_query.shape
    rows = prefill_latent.shape[0]
    heads = decode_query.shape[1]
    cache_dev = cache.shape[1]
    if head_here != 1 or n % 32 or rows * n != span or span % 512:
        raise ValueError("unexpected sizes")
    line = n // 8
    vmem = pl.BlockSpec(memory_space=pltpu.VMEM)
    anywhere = pl.BlockSpec(memory_space=pl.ANY)
    dma = pltpu.SemaphoreType.DMA
    state = pl.pallas_call(
        functools.partial(kernel, n),
        out_shape=(
            pltpu.VMEM((n // 2, 2, rows, width), jnp.bfloat16),
            pltpu.VMEM((span, width), jnp.bfloat16),
            pltpu.VMEM((span, D_LAT), jnp.float32),
            pltpu.VMEM((span, 128), jnp.float32),
            pltpu.VMEM((span, 128), jnp.float32),
            pltpu.VMEM((span, D_LAT), jnp.bfloat16),
            pltpu.VMEM((REQ, D_LAT), jnp.bfloat16),
        ),
        in_specs=[anywhere] * 6,
        out_specs=(vmem,) * 7,
        scratch_shapes=[
            pltpu.VMEM((REQ, heads, width), jnp.bfloat16),
            pltpu.VMEM((width, span), jnp.bfloat16),
            pltpu.VMEM((REQ, width, cache_dev), jnp.bfloat16),
            pltpu.SMEM(lengths.shape, jnp.int32),
            pltpu.SMEM(page_table.shape[::-1], jnp.int32),
            pltpu.VMEM((n // 2, 2, 1, REQ * MSG), jnp.float32),
            pltpu.VMEM((n // 2, 1, REQ * MSG), jnp.float32),
            pltpu.VMEM((n // 2, 1, REQ * MSG), jnp.float32),
            pltpu.VMEM((n // 2, 1, REQ * MSG), jnp.float32),
            dma((6,)),
            dma,
            dma((line,)),
            dma((line,)),
            dma((line,)),
            dma((line,)),
            dma((2,)),
            dma((2,)),
            pltpu.SemaphoreType.REGULAR((line,)),
            pltpu.SemaphoreType.REGULAR((4,)),
            pltpu.SemaphoreType.REGULAR,
        ],
        compiler_params=pltpu.CompilerParams(
            collective_id=0, has_side_effects=True, vmem_limit_bytes=VMEM_LIMIT
        ),
    )(
        prefill_query[:, 0, :].T,
        prefill_latent,
        decode_query,
        jnp.swapaxes(cache, 1, 2),
        lengths,
        page_table.T,
    )
    prefill_out, decode_out = pl.pallas_call(
        store,
        out_shape=(
            jax.ShapeDtypeStruct((span, D_LAT), jnp.bfloat16),
            jax.ShapeDtypeStruct((REQ, D_LAT), jnp.bfloat16),
        ),
        in_specs=[vmem] * 7,
        out_specs=(anywhere, anywhere),
        scratch_shapes=[pltpu.VMEM((span, D_LAT), jnp.bfloat16), dma((5,))],
        compiler_params=pltpu.CompilerParams(vmem_limit_bytes=VMEM_LIMIT),
    )(*(pltpu.with_memory_space_constraint(a, pltpu.VMEM) for a in state))
    return prefill_out[:, None, :], decode_out[:, None, :]


def solution(mesh):
    in_specs = (
        P("groups", "ctx", None),
        P(("groups", "ctx"), None),
        P("groups", None, None),
        P("groups", "ctx", None),
        P("groups"),
        P("groups", None),
    )
    out_specs = (P("groups", "ctx", None), P("groups", "ctx", None))
    return jax.shard_map(
        functools.partial(shards, mesh.shape["ctx"]),
        mesh=mesh,
        in_specs=in_specs,
        out_specs=out_specs,
        check_vma=False,
    )
```
